64 devices in a mesh: dp: 4 (over x, y), tp: 16 (over z, core).
Axes of the slice: x: 2, y: 2, z: 8, core: 2. Of those that a mesh axis runs over, the one named last changes fastest.
The devices are a block of a 4x4x8 slice.
Arguments:
- hidden: bfloat16 [64, 6, 4096], P('dp'), parts along dimension 0
- w_head: bfloat16 [4096, 128256], P(None, 'tp')
- q_draft: float32 [64, 5, 128256], P(('dp', 'tp')), parts along dimension 0
- x_draft: int32 [64, 5], P('dp'), parts along dimension 0
Outputs:
- output 1: float32 [64, 5], P(('dp', 'tp')), parts along dimension 0
- output 2: float32 [64], P(('dp', 'tp')), parts along dimension 0
- output 3: float32 [64, 5, 128256], P(('dp', 'tp')), parts along dimension 0
- output 4: float32 [64, 128256], P(('dp', 'tp')), parts along dimension 0
There are 4 independent parts. The reference program is written for one: setup_inputs(seed, part) draws one part's arguments, and reference() takes and returns one part's arrays. A program takes and returns all parts, laid end to end along the dimension named above; an argument that names none is the same for every part.
All inputs are finite; a program needn't handle non-finite values.
Results may differ from the reference program's by a relative error of at most 0.001.
Values are sent between devices in bfloat16 or wider.
A program may use at most 768 MiB of HBM per device.

```python
import jax
import jax.numpy as jnp
from jax import lax

BATCH = 16
DRAFT = 5
HIDDEN = 4096
VOCAB = 128256
INV_TEMP = 1.25


def draw_tokens(token_key):
    tokens = jax.random.randint(token_key, (BATCH, DRAFT), 0, VOCAB, dtype=jnp.int32)
    return tokens.at[0, 0].set(VOCAB - 1).at[0, 1].set(0)


def setup_inputs(seed: int = 0, part: int = 0) -> dict:
    root_key = jax.random.key(seed)
    shared_key, part_root = jax.random.split(root_key)
    part_key = jax.random.fold_in(part_root, part)
    key_hidden, key_draft, key_token = jax.random.split(part_key, 3)
    raw_hidden = jax.random.normal(key_hidden, (BATCH, DRAFT + 1, HIDDEN), jnp.float32)
    hidden = raw_hidden * lax.rsqrt(jnp.mean(raw_hidden * raw_hidden, axis=-1, keepdims=True) + 1e-6)
    w_head = jax.random.normal(shared_key, (HIDDEN, VOCAB), jnp.float32) * HIDDEN ** -0.5
    draft_logits = 1.25 * jax.random.normal(key_draft, (BATCH, DRAFT, VOCAB), jnp.float32)
    q_draft = jax.nn.softmax(draft_logits, axis=-1)
    return {"hidden": hidden.astype(jnp.bfloat16), "w_head": w_head.astype(jnp.bfloat16), "q_draft": q_draft, "x_draft": draw_tokens(key_token)}


def reference(hidden, w_head, q_draft, x_draft):
    def verify_one(seq_args):
        hidden_seq, q_seq, x_seq = seq_args
        logits = jnp.dot(hidden_seq, w_head, preferred_element_type=jnp.float32) * INV_TEMP
        row_peak = jnp.max(logits, axis=-1, keepdims=True)
        exp_vals = jnp.exp(logits - row_peak)
        target_p = exp_vals / jnp.sum(exp_vals, axis=-1, keepdims=True)
        draft_p = target_p[:DRAFT]
        p_pick = jnp.take_along_axis(draft_p, x_seq[:, None], axis=1)[:, 0]
        q_pick = jnp.take_along_axis(q_seq, x_seq[:, None], axis=1)[:, 0]
        seq_accept = jnp.minimum(1.0, p_pick / q_pick)
        seq_expected = jnp.sum(jnp.cumprod(seq_accept))
        excess = jnp.maximum(draft_p - q_seq, 0.0)
        seq_resid = excess / jnp.sum(excess, axis=-1, keepdims=True)
        return seq_accept, seq_expected, seq_resid, target_p[DRAFT]

    accept, expected, residual, bonus = lax.map(verify_one, (hidden, q_draft, x_draft))
    return accept, expected, residual, bonus
```

```python
import functools

import jax
import jax.numpy as jnp
from jax import lax
from jax.experimental import pallas as pl
from jax.experimental.pallas import tpu as pltpu
from jax.sharding import PartitionSpec as P

INV_TEMP = 1.25
LANES = 128
SUB = 8
TILE_ROWS = 2
NBUF = 4
AXIS = "tp"
MESH = pl.DeviceIdType.MESH


def exchange_kernel(geo, w_ref, h_ref, q_ref, x_ref, pe_ref, aux_ref, scale_ref,
                    hraw, hperm, ebuf, wbuf, send, recv, qbuf, stat_send, stat_recv, peak,
                    hsem, esem, wsem, qsem, ssem, rsem, tsem, usem):
    n, width, slots, pos_n, draft, batch, total_rows = geo
    f32 = jnp.float32
    me = lax.axis_index(AXIS)
    chip, core = me // 2, lax.rem(me, 2)
    chips = n // 2
    first_col = me * width
    off = pl.multiple_of(lax.rem(first_col, LANES), 16)
    last_fill = width - (slots - 1) * LANES
    slack = LANES - last_fill
    tail = pl.multiple_of(jnp.maximum(off - slack, 0), 16)
    positions = draft + 1

    hcopy = pltpu.make_async_copy(h_ref, hraw, hsem)
    hcopy.start()
    e1 = pltpu.make_async_copy(w_ref.at[pl.ds(0, LANES)], ebuf.at[pl.ds(pl.multiple_of(LANES + off, 16), LANES)], esem.at[0])
    e2 = pltpu.make_async_copy(w_ref.at[pl.ds(width - LANES, LANES)], ebuf.at[pl.ds(tail, LANES)], esem.at[1])
    want = (slots - 2) * LANES - off
    src3 = pl.multiple_of(jnp.minimum(want, width - 2 * LANES), 16)
    dst3 = pl.multiple_of(3 * LANES + slack + (src3 - want), 16)
    e3 = pltpu.make_async_copy(w_ref.at[pl.ds(src3, 2 * LANES)], ebuf.at[pl.ds(dst3, 2 * LANES)], esem.at[2])
    e1.start()
    e2.start()
    e3.start()

    tile_cols = TILE_ROWS * LANES
    tiles = (slots - 3) // TILE_ROWS

    def w_copy(t):
        start = pl.multiple_of(LANES - off + t * tile_cols, 16)
        slot = lax.rem(t, NBUF)
        return pltpu.make_async_copy(w_ref.at[pl.ds(start, tile_cols)], wbuf.at[slot], wsem.at[slot])

    for t in range(NBUF - 1):
        w_copy(t).start()

    barrier = pltpu.get_barrier_semaphore()
    for k in range(1, n):
        pl.semaphore_signal(barrier, inc=1, device_id={AXIS: lax.rem(me + k, n)}, device_id_type=MESH)

    rows_in, rows_out = positions * batch, SUB * batch
    ri = lax.broadcasted_iota(jnp.int32, (rows_out, rows_in), 0)
    ci = lax.broadcasted_iota(jnp.int32, (rows_out, rows_in), 1)
    pick = ((lax.rem(ri, SUB) * batch + ri // SUB) == ci).astype(f32).astype(jnp.bfloat16)
    hcopy.wait()
    depth = hraw.shape[1]
    hstep = 512

    @pl.loop(0, depth // hstep)
    def _(k):
        cols = pl.ds(pl.multiple_of(k * hstep, hstep), hstep)
        hperm[:, cols] = jnp.dot(pick, hraw[:, cols], preferred_element_type=f32).astype(jnp.bfloat16)

    def logits_of(block):
        z = lax.dot_general(hperm[...], block, (((1,), (1,)), ((), ())), preferred_element_type=f32)
        return z * INV_TEMP

    def put(z, pos):
        z3 = z.reshape(batch, SUB, LANES)
        send[:, pos] = z3
        return z3

    lane_e = lax.broadcasted_iota(jnp.int32, (1, 1, LANES), 2)
    ok_first = jnp.logical_or(lane_e >= off, lane_e < tail)
    ok_last = lane_e < jnp.minimum(off + last_fill, LANES)
    low = jnp.finfo(jnp.float32).min
    e1.wait()
    e2.wait()
    e3.wait()
    z_a = put(logits_of(ebuf[pl.ds(LANES, LANES), :]), 0)
    z_bc = logits_of(ebuf[pl.ds(3 * LANES + slack, 2 * LANES), :])
    z_b = put(z_bc[:, :LANES], 1)
    z_c = put(z_bc[:, LANES:], 2)
    peak[...] = jnp.maximum(jnp.where(ok_first, z_a, low), jnp.maximum(z_b, jnp.where(ok_last, z_c, low)))

    order = []
    for d in range(chips // 2, 0, -1):
        order += [(d, 0), (d, 1)]
        if 2 * d != chips:
            order += [(chips - d, 0), (chips - d, 1)]
    order.append((0, 1))

    def targets():
        for dz, dc in order:
            yield lax.rem(chip + dz, chips) * 2 + lax.rem(core + dc, 2)

    def send_group(g, pos, size):
        for tgt in targets():
            pltpu.make_async_remote_copy(
                src_ref=send.at[tgt, pl.ds(pos, size), pl.ds(0, positions), :],
                dst_ref=recv.at[me, pl.ds(pos, size), pl.ds(0, positions), :],
                send_sem=ssem.at[g], recv_sem=rsem.at[g], device_id={AXIS: tgt}, device_id_type=MESH).start()

    def keep_own(pos, size):
        for i in range(size):
            recv[me, pos + i] = send[me, pos + i]

    keep_own(0, 3)
    pl.semaphore_wait(barrier, n - 1)
    send_group(0, 0, 3)

    big = 4
    head = tiles % big
    head_rows, big_rows = head * TILE_ROWS, big * TILE_ROWS
    n_big = tiles // big
    groups = 2 + n_big
    held = 2

    @pl.loop(0, tiles)
    def _(t):
        @pl.when(t + NBUF - 1 < tiles)
        def _():
            w_copy(t + NBUF - 1).start()

        w_copy(t).wait()
        z = logits_of(wbuf[lax.rem(t, NBUF)])
        top = peak[...]
        for i in range(TILE_ROWS):
            top = jnp.maximum(top, put(z[:, i * LANES:(i + 1) * LANES], 3 + t * TILE_ROWS + i))
        peak[...] = top
        keep_own(3 + t * TILE_ROWS, TILE_ROWS)

        @pl.when(t == head - 1)
        def _():
            send_group(1, 3, head_rows)

        done = (t + 1 - head) // big

        @pl.when(jnp.logical_and(t >= head, jnp.logical_and(lax.rem(t + 1 - head, big) == 0, done <= n_big - held)))
        def _():
            send_group(1 + done, 3 + head_rows + (done - 1) * big_rows, big_rows)

    for j in range(draft):
        pltpu.make_async_copy(q_ref.at[j, :, 0, :], qbuf.at[:, j, :], qsem.at[j]).start()

    lane8 = lax.broadcasted_iota(jnp.int32, (SUB, LANES), 1)
    sub8 = lax.broadcasted_iota(jnp.int32, (SUB, LANES), 0)
    diag_m = lane8 == sub8
    diag_l = lane8 == sub8 + SUB

    @pl.loop(0, batch)
    def _(b):
        m = jnp.max(peak[b], axis=1, keepdims=True)
        acc = (jnp.where(ok_first[0], jnp.exp(send[b, 0] - m), 0.0) + jnp.exp(send[b, 1] - m)
               + jnp.where(ok_last[0], jnp.exp(send[b, 2] - m), 0.0))
        accs = [acc, jnp.zeros_like(acc), jnp.zeros_like(acc), jnp.zeros_like(acc)]
        for r in range(3, slots):
            accs[r % 4] = accs[r % 4] + jnp.exp(send[b, r] - m)
        l = jnp.sum((accs[0] + accs[1]) + (accs[2] + accs[3]), axis=1, keepdims=True)
        row = jnp.where(diag_m, m, 0.0) + jnp.where(diag_l, l, 0.0)
        stat_send[b] = jnp.sum(row, axis=0, keepdims=True)

    stat_recv[me] = stat_send[me]
    for tgt in targets():
        pltpu.make_async_remote_copy(src_ref=stat_send.at[tgt], dst_ref=stat_recv.at[me], send_sem=tsem, recv_sem=usem,
                                     device_id={AXIS: tgt}, device_id_type=MESH).start()
    for g in range(groups - held, groups):
        send_group(g, 3 + head_rows + (g - 2) * big_rows, big_rows)

    others = n - 1
    pltpu.make_async_copy(stat_recv.at[pl.ds(0, others)], stat_recv.at[pl.ds(0, others)], usem).wait()
    stats = [stat_recv[s] for s in range(n)]
    top = functools.reduce(jnp.maximum, stats)
    tot = jnp.zeros_like(top)
    for s in range(n):
        tot = tot + jnp.exp(stats[s] - top) * pltpu.roll(stats[s], LANES - SUB, 1)

    def spread(row):
        return jnp.sum(jnp.where(diag_m, row, 0.0), axis=1, keepdims=True)

    peak_g = jnp.broadcast_to(spread(top), (SUB, LANES))
    inv_sum = jnp.broadcast_to(1.0 / spread(tot), (SUB, LANES))

    for j in range(draft):
        pltpu.make_async_copy(q_ref.at[j, :, 0, :], qbuf.at[:, j, :], qsem.at[j]).wait()

    is_draft = sub8 < draft

    def excess_of(z, row):
        p = jnp.exp(z - peak_g) * inv_sum
        e = jnp.maximum(p - jnp.where(is_draft, qbuf[row], 0.0), 0.0)
        pe_ref[pl.ds(pl.multiple_of(row * SUB, SUB), SUB), :] = e
        return e

    def wait_group(g, pos, size):
        view = recv.at[pl.ds(0, others), pl.ds(pos, size), pl.ds(0, positions), :]
        pltpu.make_async_copy(view, view, rsem.at[g]).wait()

    lane_s = lane8
    parts = {}
    for s in range(n):
        first, o = (s * width) // LANES, (s * width) % LANES
        t_s = max(o - slack, 0)
        parts.setdefault(first, []).append((s, 0, o, LANES))
        if t_s:
            parts.setdefault(first + slots, []).append((s, 0, 0, t_s))
        parts.setdefault(first + slots - 1, []).append((s, 2, 0, min(LANES, o + last_fill)))
        parts.setdefault(first + slots - 2, []).append((s, 1, 0, LANES))
    wait_group(0, 0, 3)
    acc = jnp.zeros((SUB, LANES), f32)
    for row, pieces in sorted(parts.items()):
        z = recv[pieces[0][0], pieces[0][1]]
        for s, pos, lo, hi in pieces[1:]:
            z = jnp.where(jnp.logical_and(lane_s >= lo, lane_s < hi), recv[s, pos], z)
        acc = acc + excess_of(z, row)

    def main_rows(pos, size, acc):
        def one(s, acc):
            base = (s * width) // LANES + pos - 2
            es = [excess_of(recv[s, pos + i], base + i) for i in range(size)]
            while len(es) > 1:
                es = [es[i] + es[i + 1] for i in range(0, len(es) - 1, 2)] + ([es[-1]] if len(es) % 2 else [])
            return acc + es[0]
        return lax.fori_loop(0, n, one, acc)

    wait_group(1, 3, head_rows)
    acc = main_rows(3, head_rows, acc)

    def one_group(g, acc):
        pos = 3 + head_rows + (g - 2) * big_rows
        wait_group(g, pos, big_rows)
        return main_rows(pos, big_rows, acc)

    acc = lax.fori_loop(2, groups, one_group, acc)
    scale_ref[...] = jnp.broadcast_to(jnp.where(sub8[:, :1] < draft, 1.0 / jnp.sum(acc, axis=1, keepdims=True), 1.0), (SUB, LANES))

    prod = jnp.ones((1, 1), f32)
    expect = jnp.zeros((1, 1), f32)
    lane1 = lax.broadcasted_iota(jnp.int32, (1, LANES), 1)
    out_row = jnp.zeros((1, LANES), f32)
    for j in range(draft):
        x = x_ref[j, me]
        s = x // width
        row = x // LANES
        slot = row - (s * width) // LANES
        slot = jnp.where(slot == slots, 0, slot)
        pos = jnp.where(slot == 0, 0, jnp.where(slot >= slots - 2, slot - (slots - 3), slot + 2))
        here = jnp.logical_and(sub8 == j, lane8 == lax.rem(x, LANES))
        p = jnp.exp(recv[s, pos] - peak_g) * inv_sum

        def at_token(v):
            return jnp.sum(jnp.sum(jnp.where(here, v, 0.0), axis=1, keepdims=True), axis=0, keepdims=True)

        ratio = jnp.minimum(1.0, at_token(p) / at_token(qbuf[row]))
        prod = prod * ratio
        expect = expect + prod
        out_row = jnp.where(lane1 == j, ratio, out_row)
    out_row = jnp.where(lane1 == draft, expect, out_row)
    aux_ref[...] = jnp.broadcast_to(out_row, (SUB, LANES))

    def wait_sent(g, pos, size):
        view = send.at[pl.ds(0, others), pl.ds(pos, size), pl.ds(0, positions), :]
        pltpu.make_async_copy(view, view, ssem.at[g]).wait()

    wait_sent(0, 0, 3)
    wait_sent(1, 3, head_rows)

    @pl.loop(2, groups)
    def _(g):
        wait_sent(g, 3 + head_rows + (g - 2) * big_rows, big_rows)

    pltpu.make_async_copy(stat_send.at[pl.ds(0, others)], stat_send.at[pl.ds(0, others)], tsem).wait()


def finish_kernel(geo, pe_ref, scale_ref, aux_ref, res_ref, bonus_ref, acc_ref, exp_ref, stage, sem):
    total_rows, padded, draft, cuts = geo
    acc_ref[...] = aux_ref[0:1, 0:draft]
    exp_ref[...] = aux_ref[0:1, draft:draft + 1]
    scales = [jnp.broadcast_to(scale_ref[j:j + 1, :], (SUB, LANES)) for j in range(draft)]
    copies = []
    for c, (lo, hi) in enumerate(cuts):
        @pl.loop(lo // SUB, -(-hi // SUB))
        def _(k):
            for j in range(draft + 1):
                v = pe_ref[pl.ds(k * SUB * SUB + j, SUB, stride=SUB), :]
                stage[j, pl.ds(pl.multiple_of(k * SUB, SUB), SUB), :] = v * scales[j] if j < draft else v
        for j in range(draft + 1):
            dst = res_ref.at[j, pl.ds(lo, hi - lo), 0, :] if j < draft else bonus_ref.at[pl.ds(lo, hi - lo), 0, :]
            copies.append(pltpu.make_async_copy(stage.at[j, pl.ds(lo, hi - lo), :], dst, sem.at[c, j]))
            copies[-1].start()
    for cp in copies:
        cp.wait()


def solution(mesh):
    n = mesh.shape[AXIS]

    def local_step(hidden, w_shard, q_rows, x_group):
        f32 = jnp.float32
        batch, positions, depth = hidden.shape
        draft = positions - 1
        width = w_shard.shape[1]
        vocab = q_rows.shape[2]
        slots = -(-width // LANES)
        total_rows = vocab // LANES
        padded = -(-total_rows // SUB) * SUB
        slack = LANES - (width - (slots - 1) * LANES)
        h = jnp.transpose(hidden, (1, 0, 2)).reshape(positions * batch, depth)
        w = jnp.transpose(w_shard)
        q = jnp.transpose(q_rows, (1, 0, 2)).reshape(draft, total_rows, 1, LANES)
        x = jnp.transpose(x_group)
        tiles = (slots - 3) // TILE_ROWS
        groups = 2 + tiles // 4
        hbm = pl.BlockSpec(memory_space=pltpu.HBM)
        vmem = pl.BlockSpec(memory_space=pltpu.VMEM)
        geo = (n, width, slots, slots, draft, batch, total_rows)
        pe, aux, scale = pl.pallas_call(
            functools.partial(exchange_kernel, geo),
            name="verify_exchange",
            out_shape=(jax.ShapeDtypeStruct((padded * SUB, LANES), f32),
                       jax.ShapeDtypeStruct((SUB, LANES), f32),
                       jax.ShapeDtypeStruct((SUB, LANES), f32)),
            in_specs=[hbm, hbm, hbm, pl.BlockSpec(memory_space=pltpu.SMEM)],
            out_specs=(vmem, vmem, vmem),
            scratch_shapes=[
                pltpu.VMEM((positions * batch, depth), jnp.bfloat16),
                pltpu.VMEM((SUB * batch, depth), jnp.bfloat16),
                pltpu.VMEM((5 * LANES + slack, depth), jnp.bfloat16),
                pltpu.VMEM((NBUF, TILE_ROWS * LANES, depth), jnp.bfloat16),
                pltpu.VMEM((batch, slots, SUB, LANES), f32),
                pltpu.VMEM((n, slots, SUB, LANES), f32),
                pltpu.VMEM((total_rows, SUB, LANES), f32),
                pltpu.VMEM((batch, 1, LANES), f32),
                pltpu.VMEM((n, 1, LANES), f32),
                pltpu.VMEM((batch, SUB, LANES), f32),
                pltpu.SemaphoreType.DMA,
                pltpu.SemaphoreType.DMA((3,)),
                pltpu.SemaphoreType.DMA((NBUF,)),
                pltpu.SemaphoreType.DMA((draft,)),
                pltpu.SemaphoreType.DMA((groups,)),
                pltpu.SemaphoreType.DMA((groups,)),
                pltpu.SemaphoreType.DMA,
                pltpu.SemaphoreType.DMA,
            ],
            compiler_params=pltpu.CompilerParams(collective_id=0, has_side_effects=True, vmem_limit_bytes=40 * 2**20),
        )(w, h, q, x)
        step = -(-padded // 8 // SUB) * SUB
        cuts = tuple((lo, min(lo + step, total_rows)) for lo in range(0, total_rows, step))
        res, bonus, accept, expected = pl.pallas_call(
            functools.partial(finish_kernel, (total_rows, padded, draft, cuts)),
            name="verify_finish",
            out_shape=(jax.ShapeDtypeStruct((draft, total_rows, 1, LANES), f32),
                       jax.ShapeDtypeStruct((total_rows, 1, LANES), f32),
                       jax.ShapeDtypeStruct((1, draft), f32),
                       jax.ShapeDtypeStruct((1, 1), f32)),
            in_specs=[vmem, vmem, vmem],
            out_specs=(hbm, hbm, vmem, vmem),
            scratch_shapes=[pltpu.VMEM((positions, padded, LANES), f32), pltpu.SemaphoreType.DMA((len(cuts), positions))],
        )(pe, scale, aux)
        residual = jnp.transpose(res.reshape(draft, 1, vocab), (1, 0, 2))
        return accept, expected.reshape(1), residual, bonus.reshape(1, vocab)

    return jax.shard_map(local_step, mesh=mesh,
                         in_specs=(P("dp", None, None), P(None, AXIS), P(("dp", AXIS), None, None), P("dp", None)),
                         out_specs=(P(("dp", AXIS), None), P(("dp", AXIS)), P(("dp", AXIS), None, None), P(("dp", AXIS), None)),
                         check_vma=False)
```

```python
import functools

import jax
import jax.numpy as jnp
from jax import lax
from jax.experimental import pallas as pl
from jax.experimental.pallas import tpu as pltpu
from jax.sharding import PartitionSpec as P

INV_TEMP = 1.25
LANES = 128
SUB = 8
TILE_ROWS = 2
NBUF = 4
AXIS = "tp"
MESH = pl.DeviceIdType.MESH


def exchange_kernel(geo, w_ref, h_ref, q_ref, x_hbm, pe_ref,
                    x_ref, hraw, hperm, ebuf, wbuf, send, recv, qbuf, stat_send, stat_recv, peak,
                    xsem, hsem, esem, wsem, qsem, ssem, rsem, tsem, usem):
    n, width, slots, pos_n, draft, batch, total_rows = geo
    f32 = jnp.float32
    me = lax.axis_index(AXIS)
    chip, core = me // 2, lax.rem(me, 2)
    chips = n // 2
    first_col = me * width
    off = pl.multiple_of(lax.rem(first_col, LANES), 16)
    last_fill = width - (slots - 1) * LANES
    slack = LANES - last_fill
    tail = pl.multiple_of(jnp.maximum(off - slack, 0), 16)
    positions = draft + 1

    hcopy = pltpu.make_async_copy(h_ref, hraw, hsem)
    hcopy.start()
    e1 = pltpu.make_async_copy(w_ref.at[pl.ds(0, LANES)], ebuf.at[pl.ds(pl.multiple_of(LANES + off, 16), LANES)], esem.at[0])
    e2 = pltpu.make_async_copy(w_ref.at[pl.ds(width - LANES, LANES)], ebuf.at[pl.ds(tail, LANES)], esem.at[1])
    want = (slots - 2) * LANES - off
    src3 = pl.multiple_of(jnp.minimum(want, width - 2 * LANES), 16)
    dst3 = pl.multiple_of(3 * LANES + slack + (src3 - want), 16)
    e3 = pltpu.make_async_copy(w_ref.at[pl.ds(src3, 2 * LANES)], ebuf.at[pl.ds(dst3, 2 * LANES)], esem.at[2])
    e1.start()
    e2.start()
    e3.start()

    tile_cols = TILE_ROWS * LANES
    tiles = (slots - 3) // TILE_ROWS

    def w_copy(t):
        start = pl.multiple_of(LANES - off + t * tile_cols, 16)
        slot = lax.rem(t, NBUF)
        return pltpu.make_async_copy(w_ref.at[pl.ds(start, tile_cols)], wbuf.at[slot], wsem.at[slot])

    for t in range(NBUF - 1):
        w_copy(t).start()
    xcopy = pltpu.make_async_copy(x_hbm, x_ref, xsem)
    xcopy.start()

    barrier = pltpu.get_barrier_semaphore()
    for k in range(1, n):
        pl.semaphore_signal(barrier, inc=1, device_id={AXIS: lax.rem(me + k, n)}, device_id_type=MESH)

    rows_in, rows_out = positions * batch, SUB * batch
    ri = lax.broadcasted_iota(jnp.int32, (rows_out, rows_in), 0)
    ci = lax.broadcasted_iota(jnp.int32, (rows_out, rows_in), 1)
    pick = ((lax.rem(ri, SUB) * batch + ri // SUB) == ci).astype(f32).astype(jnp.bfloat16)
    hcopy.wait()
    depth = hraw.shape[1]
    hstep = 512

    @pl.loop(0, depth // hstep)
    def _(k):
        cols = pl.ds(pl.multiple_of(k * hstep, hstep), hstep)
        hperm[:, cols] = jnp.dot(pick, hraw[:, cols], preferred_element_type=f32).astype(jnp.bfloat16)

    def logits_of(block):
        z = lax.dot_general(hperm[...], block, (((1,), (1,)), ((), ())), preferred_element_type=f32)
        return z * INV_TEMP

    def put(z, pos):
        z3 = z.reshape(batch, SUB, LANES)
        send[:, pos] = z3
        return z3

    lane_e = lax.broadcasted_iota(jnp.int32, (1, 1, LANES), 2)
    ok_first = jnp.logical_or(lane_e >= off, lane_e < tail)
    ok_last = lane_e < jnp.minimum(off + last_fill, LANES)
    low = jnp.finfo(jnp.float32).min
    e1.wait()
    e2.wait()
    e3.wait()
    z_a = put(logits_of(ebuf[pl.ds(LANES, LANES), :]), 0)
    z_bc = logits_of(ebuf[pl.ds(3 * LANES + slack, 2 * LANES), :])
    z_b = put(z_bc[:, :LANES], 1)
    z_c = put(z_bc[:, LANES:], 2)
    peak[...] = jnp.maximum(jnp.where(ok_first, z_a, low), jnp.maximum(z_b, jnp.where(ok_last, z_c, low)))

    order = []
    for d in range(chips // 2, 0, -1):
        order += [(d, 0), (d, 1)]
        if 2 * d != chips:
            order += [(chips - d, 0), (chips - d, 1)]
    order.append((0, 1))

    def targets():
        for dz, dc in order:
            yield lax.rem(chip + dz, chips) * 2 + lax.rem(core + dc, 2)

    def send_group(g, pos, size):
        for tgt in targets():
            pltpu.make_async_remote_copy(
                src_ref=send.at[tgt, pl.ds(pos, size), pl.ds(0, positions), :],
                dst_ref=recv.at[me, pl.ds(pos, size), pl.ds(0, positions), :],
                send_sem=ssem.at[g], recv_sem=rsem.at[g], device_id={AXIS: tgt}, device_id_type=MESH).start()

    def keep_own(pos, size):
        for i in range(size):
            recv[me, pos + i] = send[me, pos + i]

    keep_own(0, 3)
    pl.semaphore_wait(barrier, n - 1)
    send_group(0, 0, 3)

    big = 4
    head = tiles % big
    head_rows, big_rows = head * TILE_ROWS, big * TILE_ROWS
    n_big = tiles // big
    groups = 2 + n_big
    held = 2

    @pl.loop(0, tiles)
    def _(t):
        @pl.when(t + NBUF - 1 < tiles)
        def _():
            w_copy(t + NBUF - 1).start()

        w_copy(t).wait()
        z = logits_of(wbuf[lax.rem(t, NBUF)])
        top = peak[...]
        for i in range(TILE_ROWS):
            top = jnp.maximum(top, put(z[:, i * LANES:(i + 1) * LANES], 3 + t * TILE_ROWS + i))
        peak[...] = top
        keep_own(3 + t * TILE_ROWS, TILE_ROWS)

        @pl.when(t == head - 1)
        def _():
            send_group(1, 3, head_rows)

        done = (t + 1 - head) // big

        @pl.when(jnp.logical_and(t >= head, jnp.logical_and(lax.rem(t + 1 - head, big) == 0, done <= n_big - held)))
        def _():
            send_group(1 + done, 3 + head_rows + (done - 1) * big_rows, big_rows)

    for j in range(draft):
        pltpu.make_async_copy(q_ref.at[j, :, 0, :], qbuf.at[:, j, :], qsem.at[j]).start()

    lane8 = lax.broadcasted_iota(jnp.int32, (SUB, LANES), 1)
    sub8 = lax.broadcasted_iota(jnp.int32, (SUB, LANES), 0)
    diag_m = lane8 == sub8
    diag_l = lane8 == sub8 + SUB

    @pl.loop(0, batch)
    def _(b):
        m = jnp.max(peak[b], axis=1, keepdims=True)
        acc = (jnp.where(ok_first[0], jnp.exp(send[b, 0] - m), 0.0) + jnp.exp(send[b, 1] - m)
               + jnp.where(ok_last[0], jnp.exp(send[b, 2] - m), 0.0))
        accs = [acc, jnp.zeros_like(acc), jnp.zeros_like(acc), jnp.zeros_like(acc)]
        for r in range(3, slots):
            accs[r % 4] = accs[r % 4] + jnp.exp(send[b, r] - m)
        l = jnp.sum((accs[0] + accs[1]) + (accs[2] + accs[3]), axis=1, keepdims=True)
        row = jnp.where(diag_m, m, 0.0) + jnp.where(diag_l, l, 0.0)
        stat_send[b] = jnp.sum(row, axis=0, keepdims=True)

    stat_recv[me] = stat_send[me]
    for tgt in targets():
        pltpu.make_async_remote_copy(src_ref=stat_send.at[tgt], dst_ref=stat_recv.at[me], send_sem=tsem, recv_sem=usem,
                                     device_id={AXIS: tgt}, device_id_type=MESH).start()
    for g in range(groups - held, groups):
        send_group(g, 3 + head_rows + (g - 2) * big_rows, big_rows)

    others = n - 1
    pltpu.make_async_copy(stat_recv.at[pl.ds(0, others)], stat_recv.at[pl.ds(0, others)], usem).wait()
    stats = [stat_recv[s] for s in range(n)]
    top = functools.reduce(jnp.maximum, stats)
    tot = jnp.zeros_like(top)
    for s in range(n):
        tot = tot + jnp.exp(stats[s] - top) * pltpu.roll(stats[s], LANES - SUB, 1)

    def spread(row):
        return jnp.sum(jnp.where(diag_m, row, 0.0), axis=1, keepdims=True)

    peak_g = jnp.broadcast_to(spread(top), (SUB, LANES))
    inv_sum = jnp.broadcast_to(1.0 / spread(tot), (SUB, LANES))

    for j in range(draft):
        pltpu.make_async_copy(q_ref.at[j, :, 0, :], qbuf.at[:, j, :], qsem.at[j]).wait()

    is_draft = sub8 < draft

    def excess_of(z, row):
        p = jnp.exp(z - peak_g) * inv_sum
        e = jnp.maximum(p - jnp.where(is_draft, qbuf[row], 0.0), 0.0)
        pe_ref[pl.ds(pl.multiple_of(row * SUB, SUB), SUB), :] = e
        return e

    def wait_group(g, pos, size):
        view = recv.at[pl.ds(0, others), pl.ds(pos, size), pl.ds(0, positions), :]
        pltpu.make_async_copy(view, view, rsem.at[g]).wait()

    lane_s = lane8
    parts = {}
    for s in range(n):
        first, o = (s * width) // LANES, (s * width) % LANES
        t_s = max(o - slack, 0)
        parts.setdefault(first, []).append((s, 0, o, LANES))
        if t_s:
            parts.setdefault(first + slots, []).append((s, 0, 0, t_s))
        parts.setdefault(first + slots - 1, []).append((s, 2, 0, min(LANES, o + last_fill)))
        parts.setdefault(first + slots - 2, []).append((s, 1, 0, LANES))
    wait_group(0, 0, 3)
    acc = jnp.zeros((SUB, LANES), f32)
    for row, pieces in sorted(parts.items()):
        z = recv[pieces[0][0], pieces[0][1]]
        for s, pos, lo, hi in pieces[1:]:
            z = jnp.where(jnp.logical_and(lane_s >= lo, lane_s < hi), recv[s, pos], z)
        acc = acc + excess_of(z, row)

    def main_rows(pos, size, acc):
        def one(s, acc):
            base = (s * width) // LANES + pos - 2
            es = [excess_of(recv[s, pos + i], base + i) for i in range(size)]
            while len(es) > 1:
                es = [es[i] + es[i + 1] for i in range(0, len(es) - 1, 2)] + ([es[-1]] if len(es) % 2 else [])
            return acc + es[0]
        return lax.fori_loop(0, n, one, acc)

    wait_group(1, 3, head_rows)
    acc = main_rows(3, head_rows, acc)

    def one_group(g, acc):
        pos = 3 + head_rows + (g - 2) * big_rows
        wait_group(g, pos, big_rows)
        return main_rows(pos, big_rows, acc)

    acc = lax.fori_loop(2, groups, one_group, acc)
    pe_ref[pl.ds(total_rows * SUB, SUB), :] = jnp.broadcast_to(jnp.where(sub8[:, :1] < draft, 1.0 / jnp.sum(acc, axis=1, keepdims=True), 1.0), (SUB, LANES))

    xcopy.wait()
    prod = jnp.ones((1, 1), f32)
    expect = jnp.zeros((1, 1), f32)
    lane1 = lax.broadcasted_iota(jnp.int32, (1, LANES), 1)
    out_row = jnp.zeros((1, LANES), f32)
    for j in range(draft):
        x = x_ref[j, me]
        s = x // width
        row = x // LANES
        slot = row - (s * width) // LANES
        slot = jnp.where(slot == slots, 0, slot)
        pos = jnp.where(slot == 0, 0, jnp.where(slot >= slots - 2, slot - (slots - 3), slot + 2))
        here = jnp.logical_and(sub8 == j, lane8 == lax.rem(x, LANES))
        p = jnp.exp(recv[s, pos] - peak_g) * inv_sum

        def at_token(v):
            return jnp.sum(jnp.sum(jnp.where(here, v, 0.0), axis=1, keepdims=True), axis=0, keepdims=True)

        ratio = jnp.minimum(1.0, at_token(p) / at_token(qbuf[row]))
        prod = prod * ratio
        expect = expect + prod
        out_row = jnp.where(lane1 == j, ratio, out_row)
    out_row = jnp.where(lane1 == draft, expect, out_row)
    pe_ref[pl.ds((total_rows + 1) * SUB, SUB), :] = jnp.broadcast_to(out_row, (SUB, LANES))

    def wait_sent(g, pos, size):
        view = send.at[pl.ds(0, others), pl.ds(pos, size), pl.ds(0, positions), :]
        pltpu.make_async_copy(view, view, ssem.at[g]).wait()

    wait_sent(0, 0, 3)
    wait_sent(1, 3, head_rows)

    @pl.loop(2, groups)
    def _(g):
        wait_sent(g, 3 + head_rows + (g - 2) * big_rows, big_rows)

    pltpu.make_async_copy(stat_send.at[pl.ds(0, others)], stat_send.at[pl.ds(0, others)], tsem).wait()


def finish_kernel(geo, pe_ref, res_ref, bonus_ref, acc_ref, exp_ref, stage, sem):
    total_rows, padded, draft, cuts = geo
    aux = (total_rows + 1) * SUB
    acc_ref[...] = pe_ref[aux:aux + 1, 0:draft]
    exp_ref[...] = pe_ref[aux:aux + 1, draft:draft + 1]
    scale = total_rows * SUB
    scales = [jnp.broadcast_to(pe_ref[scale + j:scale + j + 1, :], (SUB, LANES)) for j in range(draft)]
    copies = []
    for c, (lo, hi) in enumerate(cuts):
        @pl.loop(lo // SUB, -(-hi // SUB))
        def _(k):
            for j in range(draft + 1):
                v = pe_ref[pl.ds(k * SUB * SUB + j, SUB, stride=SUB), :]
                stage[j, pl.ds(pl.multiple_of(k * SUB, SUB), SUB), :] = v * scales[j] if j < draft else v
        for j in range(draft + 1):
            dst = res_ref.at[j, pl.ds(lo, hi - lo), 0, :] if j < draft else bonus_ref.at[pl.ds(lo, hi - lo), 0, :]
            copies.append(pltpu.make_async_copy(stage.at[j, pl.ds(lo, hi - lo), :], dst, sem.at[c, j]))
            copies[-1].start()
    for cp in copies:
        cp.wait()


def solution(mesh):
    n = mesh.shape[AXIS]

    def local_step(hidden, w_shard, q_rows, x_group):
        f32 = jnp.float32
        batch, positions, depth = hidden.shape
        draft = positions - 1
        width = w_shard.shape[1]
        vocab = q_rows.shape[2]
        slots = -(-width // LANES)
        total_rows = vocab // LANES
        padded = -(-(total_rows + 2) // SUB) * SUB
        slack = LANES - (width - (slots - 1) * LANES)
        h = jnp.transpose(hidden, (1, 0, 2)).reshape(positions * batch, depth)
        w = jnp.transpose(w_shard)
        q = jnp.transpose(q_rows, (1, 0, 2)).reshape(draft, total_rows, 1, LANES)
        x = jnp.transpose(x_group)
        tiles = (slots - 3) // TILE_ROWS
        groups = 2 + tiles // 4
        hbm = pl.BlockSpec(memory_space=pltpu.HBM)
        vmem = pl.BlockSpec(memory_space=pltpu.VMEM)
        geo = (n, width, slots, slots, draft, batch, total_rows)
        w, h, q, x = (pltpu.with_memory_space_constraint(a, pltpu.HBM) for a in (w, h, q, x))
        pe = pl.pallas_call(
            functools.partial(exchange_kernel, geo),
            name="verify_exchange",
            out_shape=jax.ShapeDtypeStruct((padded * SUB, LANES), f32),
            in_specs=[hbm, hbm, hbm, hbm],
            out_specs=vmem,
            scratch_shapes=[
                pltpu.SMEM((draft, batch), jnp.int32),
                pltpu.VMEM((positions * batch, depth), jnp.bfloat16),
                pltpu.VMEM((SUB * batch, depth), jnp.bfloat16),
                pltpu.VMEM((5 * LANES + slack, depth), jnp.bfloat16),
                pltpu.VMEM((NBUF, TILE_ROWS * LANES, depth), jnp.bfloat16),
                pltpu.VMEM((batch, slots, SUB, LANES), f32),
                pltpu.VMEM((n, slots, SUB, LANES), f32),
                pltpu.VMEM((total_rows, SUB, LANES), f32),
                pltpu.VMEM((batch, 1, LANES), f32),
                pltpu.VMEM((n, 1, LANES), f32),
                pltpu.VMEM((batch, SUB, LANES), f32),
                pltpu.SemaphoreType.DMA,
                pltpu.SemaphoreType.DMA,
                pltpu.SemaphoreType.DMA((3,)),
                pltpu.SemaphoreType.DMA((NBUF,)),
                pltpu.SemaphoreType.DMA((draft,)),
                pltpu.SemaphoreType.DMA((groups,)),
                pltpu.SemaphoreType.DMA((groups,)),
                pltpu.SemaphoreType.DMA,
                pltpu.SemaphoreType.DMA,
            ],
            compiler_params=pltpu.CompilerParams(collective_id=0, has_side_effects=True, vmem_limit_bytes=40 * 2**20),
        )(w, h, q, x)
        step = -(-padded // 8 // SUB) * SUB
        cuts = tuple((lo, min(lo + step, total_rows)) for lo in range(0, total_rows, step))
        res, bonus, accept, expected = pl.pallas_call(
            functools.partial(finish_kernel, (total_rows, padded, draft, cuts)),
            name="verify_finish",
            out_shape=(jax.ShapeDtypeStruct((draft, total_rows, 1, LANES), f32),
                       jax.ShapeDtypeStruct((total_rows, 1, LANES), f32),
                       jax.ShapeDtypeStruct((1, draft), f32),
                       jax.ShapeDtypeStruct((1, 1), f32)),
            in_specs=[vmem],
            out_specs=(hbm, hbm, vmem, vmem),
            scratch_shapes=[pltpu.VMEM((positions, padded, LANES), f32), pltpu.SemaphoreType.DMA((len(cuts), positions))],
            compiler_params=pltpu.CompilerParams(vmem_limit_bytes=16 * 2**20),
        )(pe)
        residual = jnp.transpose(res.reshape(draft, 1, vocab), (1, 0, 2))
        return accept, expected.reshape(1), residual, bonus.reshape(1, vocab)

    return jax.shard_map(local_step, mesh=mesh,
                         in_specs=(P("dp", None, None), P(None, AXIS), P(("dp", AXIS), None, None), P("dp", None)),
                         out_specs=(P(("dp", AXIS), None), P(("dp", AXIS)), P(("dp", AXIS), None, None), P(("dp", AXIS), None)),
                         check_vma=False)
```

```python
import functools

import jax
import jax.numpy as jnp
from jax import lax
from jax.experimental import pallas as pl
from jax.experimental.pallas import tpu as pltpu
from jax.sharding import PartitionSpec as P

INV_TEMP = 1.25
LANES = 128
SUB = 8
TILE_ROWS = 2
NBUF = 4
GROUP_TILES = 4
AXIS = "tp"
MESH = pl.DeviceIdType.MESH


def group_plan(slots):
    main = slots - 2
    plan = [(0, 1), (1, TILE_ROWS), (1 + TILE_ROWS, TILE_ROWS), (main, 2)]
    pos, rows = 1 + 2 * TILE_ROWS, GROUP_TILES * TILE_ROWS
    while pos < main:
        plan.append((pos, rows))
        pos += rows
    assert pos == main
    last, size = plan.pop()
    return plan + [(last, size - TILE_ROWS), (last + size - TILE_ROWS, TILE_ROWS)]


def exchange_kernel(geo, w_ref, h_ref, q_ref, x_hbm, pe_ref,
                    x_ref, hbuf, fbuf, ebuf, wbuf, send, recv, qbuf, stat_send, stat_recv, peak, peak_t,
                    xsem, hsem, esem, wsem, qsem, ssem, rsem, tsem, usem):
    n, width, slots, draft, batch, total_rows, pitch, plan = geo
    f32 = jnp.float32
    me = lax.axis_index(AXIS)
    chip, core = me // 2, lax.rem(me, 2)
    chips = n // 2
    off = pl.multiple_of(lax.rem(me * width, LANES), 16)
    last_fill = width - (slots - 1) * LANES
    slack = LANES - last_fill
    tail = pl.multiple_of(jnp.maximum(off - slack, 0), 16)
    positions = draft + 1
    halves = batch // SUB
    main = slots - 2
    others = n - 1
    groups = len(plan)

    hcopy = pltpu.make_async_copy(h_ref, hbuf, hsem)
    hcopy.start()
    fcopy = pltpu.make_async_copy(w_ref.at[pl.ds(pl.multiple_of(LANES - off, 16), LANES)], fbuf, esem.at[3])
    fcopy.start()

    barrier = pltpu.get_barrier_semaphore()
    for k in range(1, n):
        pl.semaphore_signal(barrier, inc=1, device_id={AXIS: lax.rem(me + k, n)}, device_id_type=MESH)

    tile_cols = TILE_ROWS * LANES
    tiles = (main - 1) // TILE_ROWS

    def w_copy(t):
        start = pl.multiple_of(2 * LANES - off + t * tile_cols, 16)
        slot = lax.rem(t, NBUF)
        return pltpu.make_async_copy(w_ref.at[pl.ds(start, tile_cols)], wbuf.at[slot], wsem.at[slot])

    w_copy(0).start()
    e1 = pltpu.make_async_copy(w_ref.at[pl.ds(0, LANES)], ebuf.at[pl.ds(pl.multiple_of(LANES + off, 16), LANES)], esem.at[0])
    e2 = pltpu.make_async_copy(w_ref.at[pl.ds(width - LANES, LANES)], ebuf.at[pl.ds(tail, LANES)], esem.at[1])
    want = (slots - 1) * LANES - off
    src3 = pl.multiple_of(jnp.minimum(want, width - LANES), 16)
    dst3 = pl.multiple_of(3 * LANES + slack + (src3 - want), 16)
    e3 = pltpu.make_async_copy(w_ref.at[pl.ds(src3, LANES)], ebuf.at[pl.ds(dst3, LANES)], esem.at[2])
    xcopy = pltpu.make_async_copy(x_hbm, x_ref, xsem)

    order = []
    for d in range(chips // 2, 0, -1):
        order += [(d, 0), (d, 1)]
        if 2 * d != chips:
            order += [(chips - d, 0), (chips - d, 1)]
    order.append((0, 1))

    def targets():
        for dz, dc in order:
            yield lax.rem(chip + dz, chips) * 2 + lax.rem(core + dc, 2)

    def send_group(g, pos, size):
        for tgt in targets():
            pltpu.make_async_remote_copy(
                src_ref=send.at[tgt, pl.ds(pos, size), pl.ds(0, positions), :],
                dst_ref=recv.at[me, pl.ds(pos, size), pl.ds(0, positions), :],
                send_sem=ssem.at[g], recv_sem=rsem.at[g], device_id={AXIS: tgt}, device_id_type=MESH).start()

    send_flat = send.reshape(batch * slots * SUB, LANES)

    def logits_of(block):
        z = lax.dot_general(hbuf[...], block, (((1,), (1,)), ((), ())), preferred_element_type=f32)
        return z * INV_TEMP

    def put(z, pos, ok=None):
        for r in range(positions * halves):
            j, half = r // halves, r % halves
            v = z[r * SUB:(r + 1) * SUB, :]
            send_flat[pl.ds((half * SUB * slots + pos) * SUB + j, SUB, stride=slots * SUB), :] = v
            peak[r] = jnp.maximum(peak[r], v if ok is None else jnp.where(ok, v, jnp.finfo(f32).min))
        recv[me, pos] = send[me, pos]

    peak[...] = jnp.full(peak.shape, jnp.finfo(f32).min, f32)
    hcopy.wait()
    fcopy.wait()
    w_copy(1).start()
    put(logits_of(fbuf[...]), 0)
    w_copy(2).start()
    e1.start()
    e2.start()
    e3.start()
    xcopy.start()
    pl.semaphore_wait(barrier, n - 1)
    send_group(0, *plan[0])

    def tile(t):
        @pl.when(t + NBUF - 1 < tiles)
        def _():
            w_copy(t + NBUF - 1).start()

        w_copy(t).wait()
        z = logits_of(wbuf[lax.rem(t, NBUF)])
        for i in range(TILE_ROWS):
            put(z[:, i * LANES:(i + 1) * LANES], 1 + t * TILE_ROWS + i)

    @pl.loop(0, 2)
    def _(t):
        tile(t)
        send_group(1 + t, 1 + t * TILE_ROWS, TILE_ROWS)

    lane8 = lax.broadcasted_iota(jnp.int32, (SUB, LANES), 1)
    sub8 = lax.broadcasted_iota(jnp.int32, (SUB, LANES), 0)
    ok_first = jnp.logical_or(lane8 >= off, lane8 < tail)
    ok_last = lane8 < jnp.minimum(off + last_fill, LANES)
    e1.wait()
    e2.wait()
    e3.wait()
    put(logits_of(ebuf[pl.ds(LANES, LANES), :]), main, ok_first)
    put(logits_of(ebuf[pl.ds(3 * LANES + slack, LANES), :]), main + 1, ok_last)
    send_group(3, *plan[3])

    big_rows = GROUP_TILES * TILE_ROWS
    held = 3

    @pl.loop(2, tiles)
    def _(t):
        tile(t)
        done = (t - 1) // GROUP_TILES

        @pl.when(jnp.logical_and(lax.rem(t - 1, GROUP_TILES) == 0, done <= groups - held - 4))
        def _():
            send_group(3 + done, 1 + 2 * TILE_ROWS + (done - 1) * big_rows, big_rows)

    for j in range(draft):
        pltpu.make_async_copy(q_ref.at[j, :, 0, :], qbuf.at[:, j, :], qsem.at[j]).start()

    diag_m = lane8 == sub8
    diag_l = lane8 == sub8 + SUB
    for r in range(positions * halves):
        peak_t[pl.ds((r % halves) * SUB * SUB + r // halves, SUB, stride=SUB), :] = peak[r]

    @pl.loop(0, batch)
    def _(b):
        m = jnp.max(peak_t[pl.ds(pl.multiple_of(b * SUB, SUB), SUB), :], axis=1, keepdims=True)
        accs = [jnp.where(ok_first, jnp.exp(send[b, main] - m), 0.0), jnp.where(ok_last, jnp.exp(send[b, main + 1] - m), 0.0),
                jnp.exp(send[b, 0] - m), jnp.exp(send[b, 1] - m)]
        for r in range(2, main):
            accs[r % 4] = accs[r % 4] + jnp.exp(send[b, r] - m)
        l = jnp.sum((accs[0] + accs[1]) + (accs[2] + accs[3]), axis=1, keepdims=True)
        row = jnp.where(diag_m, m, 0.0) + jnp.where(diag_l, l, 0.0)
        stat_send[b] = jnp.sum(row, axis=0, keepdims=True)

    stat_recv[me] = stat_send[me]
    for tgt in targets():
        pltpu.make_async_remote_copy(src_ref=stat_send.at[tgt], dst_ref=stat_recv.at[me], send_sem=tsem, recv_sem=usem,
                                     device_id={AXIS: tgt}, device_id_type=MESH).start()
    for g in range(groups - held, groups):
        send_group(g, *plan[g])

    pltpu.make_async_copy(stat_recv.at[pl.ds(0, others)], stat_recv.at[pl.ds(0, others)], usem).wait()
    stats = [stat_recv[s] for s in range(n)]
    top = functools.reduce(jnp.maximum, stats)
    tot = jnp.zeros_like(top)
    for s in range(n):
        tot = tot + jnp.exp(stats[s] - top) * pltpu.roll(stats[s], LANES - SUB, 1)

    def spread(row):
        return jnp.sum(jnp.where(diag_m, row, 0.0), axis=1, keepdims=True)

    peak_g = jnp.broadcast_to(spread(top), (SUB, LANES))
    inv_sum = jnp.broadcast_to(1.0 / spread(tot), (SUB, LANES))

    for j in range(draft):
        pltpu.make_async_copy(q_ref.at[j, :, 0, :], qbuf.at[:, j, :], qsem.at[j]).wait()
    xcopy.wait()

    is_draft = sub8 < draft

    def excess_of(z, row):
        p = jnp.exp(z - peak_g) * inv_sum
        e = jnp.maximum(p - jnp.where(is_draft, qbuf[row], 0.0), 0.0)
        pe_ref[pl.ds(row, SUB, stride=pitch), :] = e
        return e

    def wait_group(g, pos, size):
        view = recv.at[pl.ds(0, others), pl.ds(pos, size), pl.ds(0, positions), :]
        pltpu.make_async_copy(view, view, rsem.at[g]).wait()

    def main_rows(pos, size, acc):
        def one(s, acc):
            base = (s * width) // LANES + pos + 1
            es = [excess_of(recv[s, pos + i], base + i) for i in range(size)]
            while len(es) > 1:
                es = [es[i] + es[i + 1] for i in range(0, len(es) - 1, 2)] + ([es[-1]] if len(es) % 2 else [])
            return acc + es[0]
        return lax.fori_loop(0, n, one, acc)

    acc = jnp.zeros((SUB, LANES), f32)
    for g in range(3):
        wait_group(g, *plan[g])
        acc = main_rows(*plan[g], acc)

    parts = {}
    for s in range(n):
        first, o = (s * width) // LANES, (s * width) % LANES
        t_s = max(o - slack, 0)
        parts.setdefault(first, []).append((s, main, o, LANES))
        if t_s:
            parts.setdefault(first + slots, []).append((s, main, 0, t_s))
        parts.setdefault(first + slots - 1, []).append((s, main + 1, 0, min(LANES, o + last_fill)))
    wait_group(3, *plan[3])
    for row, pieces in sorted(parts.items()):
        z = recv[pieces[0][0], pieces[0][1]]
        for s, pos, lo, hi in pieces[1:]:
            z = jnp.where(jnp.logical_and(lane8 >= lo, lane8 < hi), recv[s, pos], z)
        acc = acc + excess_of(z, row)

    def one_group(g, acc):
        pos = 1 + 2 * TILE_ROWS + (g - 4) * big_rows
        wait_group(g, pos, big_rows)
        return main_rows(pos, big_rows, acc)

    acc = lax.fori_loop(4, groups - 2, one_group, acc)
    for g in range(groups - 2, groups):
        wait_group(g, *plan[g])
        acc = main_rows(*plan[g], acc)
    spare = pitch - SUB
    pe_ref[pl.ds(spare, SUB), :] = jnp.broadcast_to(1.0 / jnp.sum(acc, axis=1, keepdims=True), (SUB, LANES))

    prod = jnp.ones((1, 1), f32)
    expect = jnp.zeros((1, 1), f32)
    lane1 = lax.broadcasted_iota(jnp.int32, (1, LANES), 1)
    out_row = jnp.zeros((1, LANES), f32)
    for j in range(draft):
        x = x_ref[j, me]
        s = x // width
        row = x // LANES
        slot = row - (s * width) // LANES
        pos = jnp.where(jnp.logical_or(slot == 0, slot == slots), main, jnp.where(slot == slots - 1, main + 1, slot - 1))
        here = jnp.logical_and(sub8 == j, lane8 == lax.rem(x, LANES))
        p = jnp.exp(recv[s, pos] - peak_g) * inv_sum

        def at_token(v):
            return jnp.sum(jnp.sum(jnp.where(here, v, 0.0), axis=1, keepdims=True), axis=0, keepdims=True)

        ratio = jnp.minimum(1.0, at_token(p) / at_token(qbuf[row]))
        prod = prod * ratio
        expect = expect + prod
        out_row = jnp.where(lane1 == j, ratio, out_row)
    out_row = jnp.where(lane1 == draft, expect, out_row)
    pe_ref[pl.ds(pitch + spare, SUB), :] = jnp.broadcast_to(out_row, (SUB, LANES))

    for g in range(groups):
        pos, size = plan[g]
        view = send.at[pl.ds(0, others), pl.ds(pos, size), pl.ds(0, positions), :]
        pltpu.make_async_copy(view, view, ssem.at[g]).wait()
    pltpu.make_async_copy(stat_send.at[pl.ds(0, others)], stat_send.at[pl.ds(0, others)], tsem).wait()


def finish_kernel(geo, pe_ref, res_ref, bonus_ref, acc_ref, exp_ref, stage, sem):
    total_rows, pitch, draft, cuts = geo
    copies = [pltpu.make_async_copy(pe_ref.at[pl.ds(draft * pitch, total_rows), :], bonus_ref.at[:, 0, :], sem.at[draft * len(cuts)])]
    copies[0].start()
    spare = pitch - SUB
    for j in range(draft):
        scale = jnp.broadcast_to(pe_ref[spare + j:spare + j + 1, :], (SUB, LANES))
        for c, (lo, hi) in enumerate(cuts):
            up = -(-hi // SUB) * SUB
            block = pe_ref[j * pitch + lo:j * pitch + up, :].reshape((up - lo) // SUB, SUB, LANES)
            stage[j, lo:up, :] = (block * scale[None]).reshape(up - lo, LANES)
            copies.append(pltpu.make_async_copy(stage.at[j, pl.ds(lo, hi - lo), :], res_ref.at[j, pl.ds(lo, hi - lo), 0, :],
                                                sem.at[j * len(cuts) + c]))
            copies[-1].start()
    aux = pitch + spare
    acc_ref[...] = pe_ref[aux:aux + 1, 0:draft]
    exp_ref[...] = pe_ref[aux:aux + 1, draft:draft + 1]
    for cp in copies:
        cp.wait()


def solution(mesh):
    n = mesh.shape[AXIS]

    def local_step(hidden, w_shard, q_rows, x_group):
        f32 = jnp.float32
        batch, positions, depth = hidden.shape
        draft = positions - 1
        width = w_shard.shape[1]
        vocab = q_rows.shape[2]
        slots = -(-width // LANES)
        total_rows = vocab // LANES
        padded = -(-total_rows // SUB) * SUB
        pitch = padded + SUB
        slack = slots * LANES - width
        plan = group_plan(slots)
        groups = len(plan)
        h = jnp.transpose(hidden, (1, 0, 2)).reshape(positions * batch, depth)
        w = jnp.transpose(w_shard)
        q = jnp.transpose(q_rows, (1, 0, 2)).reshape(draft, total_rows, 1, LANES)
        x = jnp.transpose(x_group)
        hbm = pl.BlockSpec(memory_space=pltpu.HBM)
        vmem = pl.BlockSpec(memory_space=pltpu.VMEM)
        w, h, q, x = (pltpu.with_memory_space_constraint(a, pltpu.HBM) for a in (w, h, q, x))
        geo = (n, width, slots, draft, batch, total_rows, pitch, plan)
        pe = pl.pallas_call(
            functools.partial(exchange_kernel, geo),
            name="verify_exchange",
            out_shape=jax.ShapeDtypeStruct((SUB * pitch, LANES), f32),
            in_specs=[hbm, hbm, hbm, hbm],
            out_specs=vmem,
            scratch_shapes=[
                pltpu.SMEM((draft, batch), jnp.int32),
                pltpu.VMEM((positions * batch, depth), jnp.bfloat16),
                pltpu.VMEM((LANES, depth), jnp.bfloat16),
                pltpu.VMEM((4 * LANES + slack, depth), jnp.bfloat16),
                pltpu.VMEM((NBUF, TILE_ROWS * LANES, depth), jnp.bfloat16),
                pltpu.VMEM((batch, slots, SUB, LANES), f32),
                pltpu.VMEM((n, slots, SUB, LANES), f32),
                pltpu.VMEM((total_rows, SUB, LANES), f32),
                pltpu.VMEM((batch, 1, LANES), f32),
                pltpu.VMEM((n, 1, LANES), f32),
                pltpu.VMEM((positions * batch // SUB, SUB, LANES), f32),
                pltpu.VMEM((batch * SUB, LANES), f32),
                pltpu.SemaphoreType.DMA,
                pltpu.SemaphoreType.DMA,
                pltpu.SemaphoreType.DMA((4,)),
                pltpu.SemaphoreType.DMA((NBUF,)),
                pltpu.SemaphoreType.DMA((draft,)),
                pltpu.SemaphoreType.DMA((groups,)),
                pltpu.SemaphoreType.DMA((groups,)),
                pltpu.SemaphoreType.DMA,
                pltpu.SemaphoreType.DMA,
            ],
            compiler_params=pltpu.CompilerParams(collective_id=0, has_side_effects=True, vmem_limit_bytes=40 * 2**20),
        )(w, h, q, x)
        cut = padded // 2 // SUB * SUB
        cuts = ((0, cut), (cut, total_rows))
        res, bonus, accept, expected = pl.pallas_call(
            functools.partial(finish_kernel, (total_rows, pitch, draft, cuts)),
            name="verify_finish",
            out_shape=(jax.ShapeDtypeStruct((draft, total_rows, 1, LANES), f32),
                       jax.ShapeDtypeStruct((total_rows, 1, LANES), f32),
                       jax.ShapeDtypeStruct((1, draft), f32),
                       jax.ShapeDtypeStruct((1, 1), f32)),
            in_specs=[vmem],
            out_specs=(hbm, hbm, vmem, vmem),
            scratch_shapes=[pltpu.VMEM((draft, padded, LANES), f32), pltpu.SemaphoreType.DMA((draft * len(cuts) + 1,))],
            compiler_params=pltpu.CompilerParams(vmem_limit_bytes=16 * 2**20),
        )(pe)
        residual = jnp.transpose(res.reshape(draft, 1, vocab), (1, 0, 2))
        return accept, expected.reshape(1), residual, bonus.reshape(1, vocab)

    return jax.shard_map(local_step, mesh=mesh,
                         in_specs=(P("dp", None, None), P(None, AXIS), P(("dp", AXIS), None, None), P("dp", None)),
                         out_specs=(P(("dp", AXIS), None), P(("dp", AXIS)), P(("dp", AXIS), None, None), P(("dp", AXIS), None)),
                         check_vma=False)
```

```python
import functools

import jax
import jax.numpy as jnp
from jax import lax
from jax.experimental import pallas as pl
from jax.experimental.pallas import tpu as pltpu
from jax.sharding import PartitionSpec as P

INV_TEMP = 1.25
LANES = 128
SUB = 8
TILE_ROWS = 2
NBUF = 4
AXIS = "tp"
MESH = pl.DeviceIdType.MESH


GROUPS = (("F",), (1,), (2,), (4,), (8,), ("E", 7), (8,))
HELD = 2


def group_plan(slots):
    pos = tile = 0
    edge = None
    plan = []
    for group in GROUPS:
        start, first, has_edge = pos, tile, False
        for item in group:
            if item == "F":
                assert pos == 0
                pos += 1
            elif item == "E":
                assert pos == start
                edge, has_edge = pos, True
                pos += 2
            else:
                tile += item
                pos += item * TILE_ROWS
        plan.append((start, pos - start, first, tile - first, has_edge))
    assert pos == slots and edge is not None
    return tuple(plan), edge


def exchange_kernel(geo, w_ref, h_ref, q_ref, x_hbm, pe_ref,
                    x_ref, hbuf, fbuf, ebuf, wbuf, send, recv, qbuf, peak, peak_t,
                    xsem, hsem, esem, wsem, qsem, ssem, rsem, lsem):
    n, width, slots, draft, batch, total_rows, pitch, plan, edge = geo
    f32 = jnp.float32
    me = lax.axis_index(AXIS)
    chip, core = me // 2, lax.rem(me, 2)
    chips = n // 2
    off = pl.multiple_of(lax.rem(me * width, LANES), 16)
    last_fill = width - (slots - 1) * LANES
    slack = LANES - last_fill
    tail = pl.multiple_of(jnp.maximum(off - slack, 0), 16)
    positions = draft + 1
    halves = batch // SUB
    main = slots - 2
    others = n - 1
    groups = len(plan)

    hcopy = pltpu.make_async_copy(h_ref, hbuf, hsem)
    hcopy.start()
    fcopy = pltpu.make_async_copy(w_ref.at[pl.ds(pl.multiple_of(LANES - off, 16), LANES)], fbuf, esem.at[3])
    fcopy.start()

    barrier = pltpu.get_barrier_semaphore()
    for k in range(1, n):
        pl.semaphore_signal(barrier, inc=1, device_id={AXIS: lax.rem(me + k, n)}, device_id_type=MESH)

    tile_cols = TILE_ROWS * LANES
    tiles = (main - 1) // TILE_ROWS

    def w_copy(t):
        start = pl.multiple_of(2 * LANES - off + t * tile_cols, 16)
        slot = lax.rem(t, NBUF)
        return pltpu.make_async_copy(w_ref.at[pl.ds(start, tile_cols)], wbuf.at[slot], wsem.at[slot])

    w_copy(0).start()
    e1 = pltpu.make_async_copy(w_ref.at[pl.ds(0, LANES)], ebuf.at[pl.ds(pl.multiple_of(LANES + off, 16), LANES)], esem.at[0])
    e2 = pltpu.make_async_copy(w_ref.at[pl.ds(width - LANES, LANES)], ebuf.at[pl.ds(tail, LANES)], esem.at[1])
    want = (slots - 1) * LANES - off
    src3 = pl.multiple_of(jnp.minimum(want, width - LANES), 16)
    dst3 = pl.multiple_of(3 * LANES + slack + (src3 - want), 16)
    e3 = pltpu.make_async_copy(w_ref.at[pl.ds(src3, LANES)], ebuf.at[pl.ds(dst3, LANES)], esem.at[2])
    xcopy = pltpu.make_async_copy(x_hbm, x_ref, xsem)

    hops = []
    for d in range(chips // 2, 0, -1):
        hops += [d] if 2 * d == chips else [d, chips - d]
    order = [(d, c) for c in (1, 0) for d in hops] + [(0, 1)]

    def targets():
        for dz, dc in order:
            yield lax.rem(chip + dz, chips) * 2 + lax.rem(core + dc, 2)

    def send_group(g):
        pos, size = plan[g][:2]
        for k, tgt in enumerate(targets()):
            pltpu.make_async_remote_copy(
                src_ref=send.at[tgt, pl.ds(pos, size), pl.ds(0, positions), :],
                dst_ref=recv.at[me, pl.ds(pos, size), pl.ds(0, positions), :],
                send_sem=ssem.at[g], recv_sem=lsem.at[k] if g == groups - 1 else rsem.at[g], device_id={AXIS: tgt}, device_id_type=MESH).start()

    send_flat = send.reshape(batch * slots * SUB, LANES)

    def logits_of(block):
        z = lax.dot_general(hbuf[...], block, (((1,), (1,)), ((), ())), preferred_element_type=f32)
        return z * INV_TEMP

    def put(z, pos, ok=None):
        for r in range(positions * halves):
            j, half = r // halves, r % halves
            v = z[r * SUB:(r + 1) * SUB, :]
            send_flat[pl.ds((half * SUB * slots + pos) * SUB + j, SUB, stride=slots * SUB), :] = v
            peak[r] = jnp.maximum(peak[r], v if ok is None else jnp.where(ok, v, jnp.finfo(f32).min))
        recv[me, pos] = send[me, pos]

    peak[...] = jnp.full(peak.shape, jnp.finfo(f32).min, f32)
    hcopy.wait()
    fcopy.wait()
    w_copy(1).start()
    put(logits_of(fbuf[...]), 0)
    w_copy(2).start()
    e1.start()
    e2.start()
    e3.start()
    xcopy.start()

    lane8 = lax.broadcasted_iota(jnp.int32, (SUB, LANES), 1)
    sub8 = lax.broadcasted_iota(jnp.int32, (SUB, LANES), 0)
    ok_first = jnp.logical_or(lane8 >= off, lane8 < tail)
    ok_last = lane8 < jnp.minimum(off + last_fill, LANES)

    def make_group(g):
        start, _, first, count, has_edge = plan[g]
        if has_edge:
            e1.wait()
            e2.wait()
            e3.wait()
            put(logits_of(ebuf[pl.ds(LANES, LANES), :]), edge, ok_first)
            put(logits_of(ebuf[pl.ds(3 * LANES + slack, LANES), :]), edge + 1, ok_last)
        base = start + (2 if has_edge else 0) + (1 if g == 0 else 0) - first * TILE_ROWS
        if not count:
            return

        @pl.loop(first, first + count)
        def _(t):
            @pl.when(t + NBUF - 1 < tiles)
            def _():
                w_copy(t + NBUF - 1).start()

            w_copy(t).wait()
            z = logits_of(wbuf[lax.rem(t, NBUF)])
            for i in range(TILE_ROWS):
                put(z[:, i * LANES:(i + 1) * LANES], base + t * TILE_ROWS + i)

    for g in range(groups):
        make_group(g)
        if g == 0:
            pl.semaphore_wait(barrier, n - 1)
        if g < groups - HELD:
            send_group(g)

    for j in range(draft):
        pltpu.make_async_copy(q_ref.at[j, :, 0, :], qbuf.at[:, j, :], qsem.at[j]).start()

    gap_first = jnp.where(off >= slack, off - 2, LANES)
    gap_last = jnp.where(off >= slack, LANES, LANES - 2)
    for r in range(positions * halves):
        peak_t[pl.ds((r % halves) * SUB * SUB + r // halves, SUB, stride=SUB), :] = peak[r]

    @pl.loop(0, batch)
    def _(b):
        m = jnp.max(peak_t[pl.ds(pl.multiple_of(b * SUB, SUB), SUB), :], axis=1, keepdims=True)
        accs = [jnp.where(ok_first, jnp.exp(send[b, edge] - m), 0.0), jnp.where(ok_last, jnp.exp(send[b, edge + 1] - m), 0.0)] + [0.0] * 2
        for r in [r for r in range(slots) if not edge <= r < edge + 2]:
            accs[r % 4] = accs[r % 4] + jnp.exp(send[b, r] - m)
        l = jnp.sum((accs[0] + accs[1]) + (accs[2] + accs[3]), axis=1, keepdims=True)
        for at, gap in ((edge, gap_first), (edge + 1, gap_last)):
            send[b, at] = jnp.where(lane8 == gap, m, jnp.where(lane8 == gap + 1, l, send[b, at]))

    for at in (edge, edge + 1):
        recv[me, at] = send[me, at]
    for g in range(groups - HELD, groups):
        send_group(g)

    def wait_group(g):
        pos, size = plan[g][:2]
        view = recv.at[pl.ds(0, others), pl.ds(pos, size), pl.ds(0, positions), :]
        pltpu.make_async_copy(view, view, rsem.at[g]).wait()

    edge_group = next(g for g in range(groups) if plan[g][4])
    assert groups - HELD <= edge_group < groups - 1
    wait_group(edge_group)
    stats = []
    for s in range(n):
        o = (s * width) % LANES
        at, gap = (edge, o - 2) if o >= slack else (edge + 1, LANES - 2)
        v = recv[s, at]
        stats.append((v[:, gap:gap + 1], v[:, gap + 1:gap + 2]))
    top = functools.reduce(jnp.maximum, [m for m, _ in stats])
    tot = functools.reduce(jnp.add, [l * jnp.exp(m - top) for m, l in stats])
    peak_g = jnp.broadcast_to(top, (SUB, LANES))
    inv_sum = jnp.broadcast_to(1.0 / tot, (SUB, LANES))

    for j in range(draft):
        pltpu.make_async_copy(q_ref.at[j, :, 0, :], qbuf.at[:, j, :], qsem.at[j]).wait()
    xcopy.wait()

    is_draft = sub8 < draft

    def excess_of(z, row):
        p = jnp.exp(z - peak_g) * inv_sum
        e = jnp.maximum(p - jnp.where(is_draft, qbuf[row], 0.0), 0.0)
        pe_ref[pl.ds(row, SUB, stride=pitch), :] = e
        return e

    parts = {}
    for s in range(n):
        first, o = (s * width) // LANES, (s * width) % LANES
        t_s = max(o - slack, 0)
        parts.setdefault(first, []).append((s, edge, o, LANES))
        if t_s:
            parts.setdefault(first + slots, []).append((s, edge, 0, t_s))
        parts.setdefault(first + slots - 1, []).append((s, edge + 1, 0, min(LANES, o + last_fill)))

    here, where, q_at = [], [], jnp.ones((SUB, LANES), f32)
    for j in range(draft):
        x = x_ref[j, me]
        s = x // width
        row = x // LANES
        slot = row - (s * width) // LANES
        at = jnp.where(slot <= edge, slot - 1, slot + 1)
        at = jnp.where(jnp.logical_or(slot == 0, slot == slots), edge, jnp.where(slot == slots - 1, edge + 1, at))
        where.append((s, at))
        here.append(jnp.logical_and(sub8 == j, lane8 == lax.rem(x, LANES)))
        q_at = jnp.where(here[j], qbuf[row], q_at)
    spare = pitch - SUB
    chosen = functools.reduce(jnp.logical_or, here)
    for i, v in enumerate((q_at, jnp.where(chosen, 1.0, 0.0), peak_g, inv_sum)):
        pe_ref[pl.ds((2 + i) * pitch + spare, SUB), :] = v

    def rows_of(s, pos, size, acc):
        base = (s * width) // LANES + pos + (1 if pos < edge else -1)
        es = [excess_of(recv[s, pos + i], base + i) for i in range(size)]
        while len(es) > 1:
            es = [es[i] + es[i + 1] for i in range(0, len(es) - 1, 2)] + ([es[-1]] if len(es) % 2 else [])
        return acc + es[0]

    acc = jnp.zeros((SUB, LANES), f32)
    for g in range(groups - 1):
        pos, size, _, _, has_edge = plan[g]
        if has_edge:
            for row, pieces in sorted(parts.items()):
                z = recv[pieces[0][0], pieces[0][1]]
                for s, at, lo, hi in pieces[1:]:
                    z = jnp.where(jnp.logical_and(lane8 >= lo, lane8 < hi), recv[s, at], z)
                acc = acc + excess_of(z, row)
            pos, size = pos + 2, size - 2
        else:
            wait_group(g)
        if size:
            acc = lax.fori_loop(0, n, functools.partial(lambda s, acc, pos, size: rows_of(s, pos, size, acc), pos=pos, size=size), acc)

    pos, size = plan[groups - 1][:2]
    acc = rows_of(me, pos, size, acc)
    for k, (dz, dc) in enumerate(order):
        s = lax.rem(chip - dz + chips, chips) * 2 + lax.rem(core + dc, 2)
        view = recv.at[s, pl.ds(pos, size), pl.ds(0, positions), :]
        pltpu.make_async_copy(view, view, lsem.at[k]).wait()
        acc = rows_of(s, pos, size, acc)
    pe_ref[pl.ds(spare, SUB), :] = jnp.broadcast_to(1.0 / jnp.sum(acc, axis=1, keepdims=True), (SUB, LANES))
    z_at = jnp.zeros((SUB, LANES), f32)
    for j in range(draft):
        z_at = jnp.where(here[j], recv[where[j][0], where[j][1]], z_at)
    pe_ref[pl.ds(pitch + spare, SUB), :] = z_at

    for g in range(groups):
        pos, size = plan[g][:2]
        view = send.at[pl.ds(0, others), pl.ds(pos, size), pl.ds(0, positions), :]
        pltpu.make_async_copy(view, view, ssem.at[g]).wait()


def finish_kernel(geo, pe_ref, res_ref, bonus_ref, acc_ref, exp_ref, stage, sem):
    total_rows, pitch, draft, cuts = geo
    copies = [pltpu.make_async_copy(pe_ref.at[pl.ds(draft * pitch, total_rows), :], bonus_ref.at[:, 0, :], sem.at[draft * len(cuts)])]
    copies[0].start()
    spare = pitch - SUB
    for j in range(draft):
        scale = jnp.broadcast_to(pe_ref[spare + j:spare + j + 1, :], (SUB, LANES))
        for c, (lo, hi) in enumerate(cuts):
            up = -(-hi // SUB) * SUB
            block = pe_ref[j * pitch + lo:j * pitch + up, :].reshape((up - lo) // SUB, SUB, LANES)
            stage[j, lo:up, :] = (block * scale[None]).reshape(up - lo, LANES)
            copies.append(pltpu.make_async_copy(stage.at[j, pl.ds(lo, hi - lo), :], res_ref.at[j, pl.ds(lo, hi - lo), 0, :],
                                                sem.at[j * len(cuts) + c]))
            copies[-1].start()
    z_at, q_at, chosen, peak_g, inv_sum = (pe_ref[(1 + i) * pitch + spare:(2 + i) * pitch, :] for i in range(5))
    ratio = jnp.minimum(1.0, jnp.exp(z_at - peak_g) * inv_sum / q_at)
    accept = jnp.sum(jnp.where(chosen > 0.5, ratio, 0.0), axis=1, keepdims=True)
    lane8 = lax.broadcasted_iota(jnp.int32, (SUB, LANES), 1)
    sub8 = lax.broadcasted_iota(jnp.int32, (SUB, LANES), 0)
    acc_ref[...] = jnp.sum(jnp.where(lane8 == sub8, accept, 0.0), axis=0, keepdims=True)[:, :draft]
    prod = accept[0:1, :]
    expect = prod
    for j in range(1, draft):
        prod = prod * accept[j:j + 1, :]
        expect = expect + prod
    exp_ref[...] = expect
    for cp in copies:
        cp.wait()


def solution(mesh):
    n = mesh.shape[AXIS]

    def local_step(hidden, w_shard, q_rows, x_group):
        f32 = jnp.float32
        batch, positions, depth = hidden.shape
        draft = positions - 1
        width = w_shard.shape[1]
        vocab = q_rows.shape[2]
        slots = -(-width // LANES)
        total_rows = vocab // LANES
        padded = -(-total_rows // SUB) * SUB
        pitch = padded + SUB
        slack = slots * LANES - width
        plan, edge = group_plan(slots)
        groups = len(plan)
        h = jnp.transpose(hidden, (1, 0, 2)).reshape(positions * batch, depth)
        w = jnp.transpose(w_shard)
        q = jnp.transpose(q_rows, (1, 0, 2)).reshape(draft, total_rows, 1, LANES)
        x = jnp.transpose(x_group)
        hbm = pl.BlockSpec(memory_space=pltpu.HBM)
        vmem = pl.BlockSpec(memory_space=pltpu.VMEM)
        w, h, q, x = (pltpu.with_memory_space_constraint(a, pltpu.HBM) for a in (w, h, q, x))
        geo = (n, width, slots, draft, batch, total_rows, pitch, plan, edge)
        pe = pl.pallas_call(
            functools.partial(exchange_kernel, geo),
            name="verify_exchange",
            out_shape=jax.ShapeDtypeStruct((SUB * pitch, LANES), f32),
            in_specs=[hbm, hbm, hbm, hbm],
            out_specs=vmem,
            scratch_shapes=[
                pltpu.SMEM((draft, batch), jnp.int32),
                pltpu.VMEM((positions * batch, depth), jnp.bfloat16),
                pltpu.VMEM((LANES, depth), jnp.bfloat16),
                pltpu.VMEM((4 * LANES + slack, depth), jnp.bfloat16),
                pltpu.VMEM((NBUF, TILE_ROWS * LANES, depth), jnp.bfloat16),
                pltpu.VMEM((batch, slots, SUB, LANES), f32),
                pltpu.VMEM((n, slots, SUB, LANES), f32),
                pltpu.VMEM((total_rows, SUB, LANES), f32),
                pltpu.VMEM((positions * batch // SUB, SUB, LANES), f32),
                pltpu.VMEM((batch * SUB, LANES), f32),
                pltpu.SemaphoreType.DMA,
                pltpu.SemaphoreType.DMA,
                pltpu.SemaphoreType.DMA((4,)),
                pltpu.SemaphoreType.DMA((NBUF,)),
                pltpu.SemaphoreType.DMA((draft,)),
                pltpu.SemaphoreType.DMA((groups,)),
                pltpu.SemaphoreType.DMA((groups,)),
                pltpu.SemaphoreType.DMA((n - 1,)),
            ],
            compiler_params=pltpu.CompilerParams(collective_id=0, has_side_effects=True, vmem_limit_bytes=40 * 2**20),
        )(w, h, q, x)
        cuts = ((0, total_rows),)
        res, bonus, accept, expected = pl.pallas_call(
            functools.partial(finish_kernel, (total_rows, pitch, draft, cuts)),
            name="verify_finish",
            out_shape=(jax.ShapeDtypeStruct((draft, total_rows, 1, LANES), f32),
                       jax.ShapeDtypeStruct((total_rows, 1, LANES), f32),
                       jax.ShapeDtypeStruct((1, draft), f32),
                       jax.ShapeDtypeStruct((1, 1), f32)),
            in_specs=[vmem],
            out_specs=(hbm, hbm, vmem, vmem),
            scratch_shapes=[pltpu.VMEM((draft, padded, LANES), f32), pltpu.SemaphoreType.DMA((draft * len(cuts) + 1,))],
            compiler_params=pltpu.CompilerParams(vmem_limit_bytes=16 * 2**20),
        )(pe)
        residual = jnp.transpose(res.reshape(draft, 1, vocab), (1, 0, 2))
        return accept, expected.reshape(1), residual, bonus.reshape(1, vocab)

    return jax.shard_map(local_step, mesh=mesh,
                         in_specs=(P("dp", None, None), P(None, AXIS), P(("dp", AXIS), None, None), P("dp", None)),
                         out_specs=(P(("dp", AXIS), None), P(("dp", AXIS)), P(("dp", AXIS), None, None), P(("dp", AXIS), None)),
                         check_vma=False)
```

```python
import functools

import jax
import jax.numpy as jnp
from jax import lax
from jax.experimental import pallas as pl
from jax.experimental.pallas import tpu as pltpu
from jax.sharding import PartitionSpec as P

INV_TEMP = 1.25
LANES = 128
SUB = 8
TILE_ROWS = 2
NBUF = 4
AXIS = "tp"
MESH = pl.DeviceIdType.MESH


GROUPS = (("F",), (1,), (1,), (2,), (4,), (8,), ("E", 7), (7,))
HELD = 2
LAST_SHARE = 4


def group_plan(slots):
    pos = tile = 0
    edge = None
    plan = []
    for group in GROUPS:
        start, first, has_edge = pos, tile, False
        for item in group:
            if item == "F":
                assert pos == 0
                pos += 1
            elif item == "E":
                assert pos == start
                edge, has_edge = pos, True
                pos += 2
            else:
                tile += item
                pos += item * TILE_ROWS
        plan.append((start, pos - start, first, tile - first, has_edge))
    assert pos == slots and edge is not None
    return tuple(plan), edge


def exchange_kernel(geo, w_ref, h_ref, q_ref, x_hbm, pe_ref,
                    x_ref, hbuf, fbuf, ebuf, wbuf, send, recv, qbuf, peak, peak_t,
                    xsem, hsem, esem, wsem, qsem, ssem, rsem, lsem):
    n, width, slots, draft, batch, total_rows, pitch, plan, edge = geo
    f32 = jnp.float32
    me = lax.axis_index(AXIS)
    chip, core = me // 2, lax.rem(me, 2)
    chips = n // 2
    off = pl.multiple_of(lax.rem(me * width, LANES), 16)
    last_fill = width - (slots - 1) * LANES
    slack = LANES - last_fill
    tail = pl.multiple_of(jnp.maximum(off - slack, 0), 16)
    positions = draft + 1
    halves = batch // SUB
    main = slots - 2
    others = n - 1
    groups = len(plan)

    hcopy = pltpu.make_async_copy(h_ref, hbuf, hsem)
    hcopy.start()
    fcopy = pltpu.make_async_copy(w_ref.at[pl.ds(pl.multiple_of(LANES - off, 16), LANES)], fbuf, hsem)
    fcopy.start()

    barrier = pltpu.get_barrier_semaphore()
    for k in range(1, n):
        pl.semaphore_signal(barrier, inc=1, device_id={AXIS: lax.rem(me + k, n)}, device_id_type=MESH)

    tile_cols = TILE_ROWS * LANES
    tiles = (main - 1) // TILE_ROWS

    def w_copy(t):
        start = pl.multiple_of(2 * LANES - off + t * tile_cols, 16)
        slot = lax.rem(t, NBUF)
        return pltpu.make_async_copy(w_ref.at[pl.ds(start, tile_cols)], wbuf.at[slot], wsem.at[slot])

    w_copy(0).start()
    e1 = pltpu.make_async_copy(w_ref.at[pl.ds(0, LANES)], ebuf.at[pl.ds(pl.multiple_of(LANES + off, 16), LANES)], esem)
    e2 = pltpu.make_async_copy(w_ref.at[pl.ds(width - LANES, LANES)], ebuf.at[pl.ds(tail, LANES)], esem)
    want = (slots - 1) * LANES - off
    src3 = pl.multiple_of(jnp.minimum(want, width - LANES), 16)
    dst3 = pl.multiple_of(3 * LANES + slack + (src3 - want), 16)
    e3 = pltpu.make_async_copy(w_ref.at[pl.ds(src3, LANES)], ebuf.at[pl.ds(dst3, LANES)], esem)
    xcopy = pltpu.make_async_copy(x_hbm, x_ref, xsem)

    hops = []
    for d in range(chips // 2, 0, -1):
        hops += [d] if 2 * d == chips else [d, chips - d]
    order = [(d, c) for c in (1, 0) for d in hops] + [(0, 1)]

    def targets():
        for dz, dc in order:
            yield lax.rem(chip + dz, chips) * 2 + lax.rem(core + dc, 2)

    def send_group(g):
        pos, size = plan[g][:2]
        for k, tgt in enumerate(targets()):
            pltpu.make_async_remote_copy(
                src_ref=send.at[tgt, pl.ds(pos, size), pl.ds(0, positions), :],
                dst_ref=recv.at[me, pl.ds(pos, size), pl.ds(0, positions), :],
                send_sem=ssem, recv_sem=lsem.at[k // LAST_SHARE] if g == groups - 1 else rsem, device_id={AXIS: tgt}, device_id_type=MESH).start()

    send_flat = send.reshape(batch * slots * SUB, LANES)

    def logits_of(block):
        z = lax.dot_general(hbuf[...], block, (((1,), (1,)), ((), ())), preferred_element_type=f32)
        return z * INV_TEMP

    def put(z, pos, ok=None):
        for r in range(positions * halves):
            j, half = r // halves, r % halves
            v = z[r * SUB:(r + 1) * SUB, :]
            send_flat[pl.ds((half * SUB * slots + pos) * SUB + j, SUB, stride=slots * SUB), :] = v
            peak[r] = jnp.maximum(peak[r], v if ok is None else jnp.where(ok, v, jnp.finfo(f32).min))
        recv[me, pos] = send[me, pos]

    peak[...] = jnp.full(peak.shape, jnp.finfo(f32).min, f32)
    both = ebuf.at[pl.ds(0, hbuf.shape[0] + LANES)]
    pltpu.make_async_copy(both, both, hsem).wait()
    w_copy(1).start()
    put(logits_of(fbuf[...]), 0)
    w_copy(2).start()
    e1.start()
    e2.start()
    e3.start()
    xcopy.start()

    lane8 = lax.broadcasted_iota(jnp.int32, (SUB, LANES), 1)
    sub8 = lax.broadcasted_iota(jnp.int32, (SUB, LANES), 0)
    ok_first = jnp.logical_or(lane8 >= off, lane8 < tail)
    ok_last = lane8 < jnp.minimum(off + last_fill, LANES)

    def make_group(g):
        start, _, first, count, has_edge = plan[g]
        if has_edge:
            three = ebuf.at[pl.ds(0, 3 * LANES)]
            pltpu.make_async_copy(three, three, esem).wait()
            put(logits_of(ebuf[pl.ds(LANES, LANES), :]), edge, ok_first)
            put(logits_of(ebuf[pl.ds(3 * LANES + slack, LANES), :]), edge + 1, ok_last)
        base = start + (2 if has_edge else 0) + (1 if g == 0 else 0) - first * TILE_ROWS
        if not count:
            return

        @pl.loop(first, first + count)
        def _(t):
            @pl.when(t + NBUF - 1 < tiles)
            def _():
                w_copy(t + NBUF - 1).start()

            w_copy(t).wait()
            z = logits_of(wbuf[lax.rem(t, NBUF)])
            for i in range(TILE_ROWS):
                put(z[:, i * LANES:(i + 1) * LANES], base + t * TILE_ROWS + i)

    for g in range(groups):
        make_group(g)
        if g == 0:
            pl.semaphore_wait(barrier, n - 1)
        if g < groups - HELD:
            send_group(g)

    for j in range(draft):
        pltpu.make_async_copy(q_ref.at[j, :, 0, :], qbuf.at[:, j, :], qsem).start()

    gap_first = jnp.where(off >= slack, off - 2, LANES)
    gap_last = jnp.where(off >= slack, LANES, LANES - 2)
    for r in range(positions * halves):
        peak_t[pl.ds((r % halves) * SUB * SUB + r // halves, SUB, stride=SUB), :] = peak[r]

    @pl.loop(0, batch)
    def _(b):
        m = jnp.max(peak_t[pl.ds(pl.multiple_of(b * SUB, SUB), SUB), :], axis=1, keepdims=True)
        accs = [jnp.where(ok_first, jnp.exp(send[b, edge] - m), 0.0), jnp.where(ok_last, jnp.exp(send[b, edge + 1] - m), 0.0)] + [0.0] * 2
        for r in [r for r in range(slots) if not edge <= r < edge + 2]:
            accs[r % 4] = accs[r % 4] + jnp.exp(send[b, r] - m)
        l = jnp.sum((accs[0] + accs[1]) + (accs[2] + accs[3]), axis=1, keepdims=True)
        for at, gap in ((edge, gap_first), (edge + 1, gap_last)):
            send[b, at] = jnp.where(lane8 == gap, m, jnp.where(lane8 == gap + 1, l, send[b, at]))

    for at in (edge, edge + 1):
        recv[me, at] = send[me, at]
    for g in range(groups - HELD, groups):
        send_group(g)

    edge_group = next(g for g in range(groups) if plan[g][4])
    assert groups - HELD <= edge_group == groups - 2
    pos, size = plan[groups - 1][:2]
    assert pos + size == slots
    early = recv.at[pl.ds(0, others), pl.ds(0, pos), pl.ds(0, positions), :]
    pltpu.make_async_copy(early, early, rsem).wait()
    stats = []
    for s in range(n):
        o = (s * width) % LANES
        at, gap = (edge, o - 2) if o >= slack else (edge + 1, LANES - 2)
        v = recv[s, at]
        stats.append((v[:, gap:gap + 1], v[:, gap + 1:gap + 2]))
    top = functools.reduce(jnp.maximum, [m for m, _ in stats])
    tot = functools.reduce(jnp.add, [l * jnp.exp(m - top) for m, l in stats])
    peak_g = jnp.broadcast_to(top, (SUB, LANES))
    inv_sum = jnp.broadcast_to(1.0 / tot, (SUB, LANES))

    every = qbuf.at[:, pl.ds(0, draft), :]
    pltpu.make_async_copy(every, every, qsem).wait()
    xcopy.wait()

    is_draft = sub8 < draft

    def excess_of(z, row):
        p = jnp.exp(z - peak_g) * inv_sum
        e = jnp.maximum(p - jnp.where(is_draft, qbuf[row], 0.0), 0.0)
        pe_ref[pl.ds(row, SUB, stride=pitch), :] = e
        return e

    parts = {}
    for s in range(n):
        first, o = (s * width) // LANES, (s * width) % LANES
        t_s = max(o - slack, 0)
        parts.setdefault(first, []).append((s, edge, o, LANES))
        if t_s:
            parts.setdefault(first + slots, []).append((s, edge, 0, t_s))
        parts.setdefault(first + slots - 1, []).append((s, edge + 1, 0, min(LANES, o + last_fill)))

    here, where, q_at = [], [], jnp.ones((SUB, LANES), f32)
    for j in range(draft):
        x = x_ref[j, me]
        s = x // width
        row = x // LANES
        slot = row - (s * width) // LANES
        at = jnp.where(slot <= edge, slot - 1, slot + 1)
        at = jnp.where(jnp.logical_or(slot == 0, slot == slots), edge, jnp.where(slot == slots - 1, edge + 1, at))
        where.append((s, at))
        here.append(jnp.logical_and(sub8 == j, lane8 == lax.rem(x, LANES)))
        q_at = jnp.where(here[j], qbuf[row], q_at)
    spare = pitch - SUB
    chosen = functools.reduce(jnp.logical_or, here)
    for i, v in enumerate((q_at, jnp.where(chosen, 1.0, 0.0), peak_g, inv_sum)):
        pe_ref[pl.ds((2 + i) * pitch + spare, SUB), :] = v

    def rows_of(s, pos, size, acc):
        base = (s * width) // LANES + pos + (1 if pos < edge else -1)
        es = [excess_of(recv[s, pos + i], base + i) for i in range(size)]
        while len(es) > 1:
            es = [es[i] + es[i + 1] for i in range(0, len(es) - 1, 2)] + ([es[-1]] if len(es) % 2 else [])
        return acc + es[0]

    acc = jnp.zeros((SUB, LANES), f32)
    for g in range(groups - 1):
        pos, size, _, _, has_edge = plan[g]
        if has_edge:
            for row, pieces in sorted(parts.items()):
                z = recv[pieces[0][0], pieces[0][1]]
                for s, at, lo, hi in pieces[1:]:
                    z = jnp.where(jnp.logical_and(lane8 >= lo, lane8 < hi), recv[s, at], z)
                acc = acc + excess_of(z, row)
            pos, size = pos + 2, size - 2
        if size:
            acc = lax.fori_loop(0, n, functools.partial(lambda s, acc, pos, size: rows_of(s, pos, size, acc), pos=pos, size=size), acc)

    pos, size = plan[groups - 1][:2]
    acc = rows_of(me, pos, size, acc)
    for k, (dz, dc) in enumerate(order):
        if k % LAST_SHARE == 0:
            view = recv.at[pl.ds(0, min(LAST_SHARE, others - k)), pl.ds(pos, size), pl.ds(0, positions), :]
            pltpu.make_async_copy(view, view, lsem.at[k // LAST_SHARE]).wait()
        acc = rows_of(lax.rem(chip - dz + chips, chips) * 2 + lax.rem(core + dc, 2), pos, size, acc)
    pe_ref[pl.ds(spare, SUB), :] = jnp.broadcast_to(1.0 / jnp.sum(acc, axis=1, keepdims=True), (SUB, LANES))
    z_at = jnp.zeros((SUB, LANES), f32)
    for j in range(draft):
        z_at = jnp.where(here[j], recv[where[j][0], where[j][1]], z_at)
    pe_ref[pl.ds(pitch + spare, SUB), :] = z_at

    sent = send.at[pl.ds(0, others), :, pl.ds(0, positions), :]
    pltpu.make_async_copy(sent, sent, ssem).wait()


def finish_kernel(geo, pe_ref, res_ref, bonus_ref, acc_ref, exp_ref, stage, sem):
    total_rows, pitch, draft, cuts = geo
    copies = [pltpu.make_async_copy(pe_ref.at[pl.ds(draft * pitch, total_rows), :], bonus_ref.at[:, 0, :], sem)]
    copies[0].start()
    spare = pitch - SUB
    for j in range(draft):
        scale = jnp.broadcast_to(pe_ref[spare + j:spare + j + 1, :], (SUB, LANES))
        for lo, hi in cuts:
            up = -(-hi // SUB) * SUB
            block = pe_ref[j * pitch + lo:j * pitch + up, :].reshape((up - lo) // SUB, SUB, LANES)
            stage[j, lo:up, :] = (block * scale[None]).reshape(up - lo, LANES)
            copies.append(pltpu.make_async_copy(stage.at[j, pl.ds(lo, hi - lo), :], res_ref.at[j, pl.ds(lo, hi - lo), 0, :], sem))
            copies[-1].start()
    z_at, q_at, chosen, peak_g, inv_sum = (pe_ref[(1 + i) * pitch + spare:(2 + i) * pitch, :] for i in range(5))
    ratio = jnp.minimum(1.0, jnp.exp(z_at - peak_g) * inv_sum / q_at)
    accept = jnp.sum(jnp.where(chosen > 0.5, ratio, 0.0), axis=1, keepdims=True)
    lane8 = lax.broadcasted_iota(jnp.int32, (SUB, LANES), 1)
    sub8 = lax.broadcasted_iota(jnp.int32, (SUB, LANES), 0)
    acc_ref[...] = jnp.sum(jnp.where(lane8 == sub8, accept, 0.0), axis=0, keepdims=True)[:, :draft]
    prod = accept[0:1, :]
    expect = prod
    for j in range(1, draft):
        prod = prod * accept[j:j + 1, :]
        expect = expect + prod
    exp_ref[...] = expect
    whole = pe_ref.at[pl.ds(0, (draft + 1) * total_rows), :]
    pltpu.make_async_copy(whole, whole, sem).wait()


def solution(mesh):
    n = mesh.shape[AXIS]

    def local_step(hidden, w_shard, q_rows, x_group):
        f32 = jnp.float32
        batch, positions, depth = hidden.shape
        draft = positions - 1
        width = w_shard.shape[1]
        vocab = q_rows.shape[2]
        slots = -(-width // LANES)
        total_rows = vocab // LANES
        padded = -(-total_rows // SUB) * SUB
        pitch = padded + SUB
        slack = slots * LANES - width
        plan, edge = group_plan(slots)
        h = jnp.transpose(hidden, (1, 0, 2)).reshape(positions * batch, depth)
        w = jnp.transpose(w_shard)
        q = jnp.transpose(q_rows, (1, 0, 2)).reshape(draft, total_rows, 1, LANES)
        x = jnp.transpose(x_group)
        hbm = pl.BlockSpec(memory_space=pltpu.HBM)
        vmem = pl.BlockSpec(memory_space=pltpu.VMEM)
        w, h, q, x = (pltpu.with_memory_space_constraint(a, pltpu.HBM) for a in (w, h, q, x))
        geo = (n, width, slots, draft, batch, total_rows, pitch, plan, edge)
        pe = pl.pallas_call(
            functools.partial(exchange_kernel, geo),
            name="verify_exchange",
            out_shape=jax.ShapeDtypeStruct((SUB * pitch, LANES), f32),
            in_specs=[hbm, hbm, hbm, hbm],
            out_specs=vmem,
            scratch_shapes=[
                pltpu.SMEM((draft, batch), jnp.int32),
                pltpu.VMEM((positions * batch, depth), jnp.bfloat16),
                pltpu.VMEM((LANES, depth), jnp.bfloat16),
                pltpu.VMEM((4 * LANES + slack, depth), jnp.bfloat16),
                pltpu.VMEM((NBUF, TILE_ROWS * LANES, depth), jnp.bfloat16),
                pltpu.VMEM((batch, slots, SUB, LANES), f32),
                pltpu.VMEM((n, slots, SUB, LANES), f32),
                pltpu.VMEM((total_rows, SUB, LANES), f32),
                pltpu.VMEM((positions * batch // SUB, SUB, LANES), f32),
                pltpu.VMEM((batch * SUB, LANES), f32),
                pltpu.SemaphoreType.DMA,
                pltpu.SemaphoreType.DMA,
                pltpu.SemaphoreType.DMA,
                pltpu.SemaphoreType.DMA((NBUF,)),
                pltpu.SemaphoreType.DMA,
                pltpu.SemaphoreType.DMA,
                pltpu.SemaphoreType.DMA,
                pltpu.SemaphoreType.DMA((-(-(n - 1) // LAST_SHARE),)),
            ],
            compiler_params=pltpu.CompilerParams(collective_id=0, has_side_effects=True, vmem_limit_bytes=40 * 2**20),
        )(w, h, q, x)
        cuts = ((0, total_rows),)
        res, bonus, accept, expected = pl.pallas_call(
            functools.partial(finish_kernel, (total_rows, pitch, draft, cuts)),
            name="verify_finish",
            out_shape=(jax.ShapeDtypeStruct((draft, total_rows, 1, LANES), f32),
                       jax.ShapeDtypeStruct((total_rows, 1, LANES), f32),
                       jax.ShapeDtypeStruct((1, draft), f32),
                       jax.ShapeDtypeStruct((1, 1), f32)),
            in_specs=[vmem],
            out_specs=(hbm, hbm, vmem, vmem),
            scratch_shapes=[pltpu.VMEM((draft, padded, LANES), f32), pltpu.SemaphoreType.DMA],
            compiler_params=pltpu.CompilerParams(vmem_limit_bytes=16 * 2**20),
        )(pe)
        residual = jnp.transpose(res.reshape(draft, 1, vocab), (1, 0, 2))
        return accept, expected.reshape(1), residual, bonus.reshape(1, vocab)

    return jax.shard_map(local_step, mesh=mesh,
                         in_specs=(P("dp", None, None), P(None, AXIS), P(("dp", AXIS), None, None), P("dp", None)),
                         out_specs=(P(("dp", AXIS), None), P(("dp", AXIS)), P(("dp", AXIS), None, None), P(("dp", AXIS), None)),
                         check_vma=False)
```

```python
import functools

import jax
import jax.numpy as jnp
from jax import lax
from jax.experimental import pallas as pl
from jax.experimental.pallas import tpu as pltpu
from jax.sharding import PartitionSpec as P

INV_TEMP = 1.25
LANES = 128
SUB = 8
TILE_ROWS = 2
NBUF = 4
AXIS = "tp"
MESH = pl.DeviceIdType.MESH


GROUPS = (("F",), (1,), (1,), (2,), (4,), (8,), ("E", 8), (6,))
HELD = 2
LAST_SHARE = 4


def group_plan(slots):
    pos = tile = 0
    edge = None
    plan = []
    for group in GROUPS:
        start, first, has_edge = pos, tile, False
        for item in group:
            if item == "F":
                assert pos == 0
                pos += 1
            elif item == "E":
                assert pos == start
                edge, has_edge = pos, True
                pos += 2
            else:
                tile += item
                pos += item * TILE_ROWS
        plan.append((start, pos - start, first, tile - first, has_edge))
    assert pos == slots and edge is not None
    return tuple(plan), edge


def exchange_kernel(geo, w_ref, h_ref, q_ref, x_hbm, pe_ref,
                    x_ref, hbuf, fbuf, ebuf, wbuf, send, recv, qbuf, peak, peak_t,
                    xsem, hsem, esem, wsem, qsem, ssem, rsem, lsem):
    n, width, slots, draft, batch, total_rows, pitch, plan, edge = geo
    f32 = jnp.float32
    me = lax.axis_index(AXIS)
    chip, core = me // 2, lax.rem(me, 2)
    chips = n // 2
    off = pl.multiple_of(lax.rem(me * width, LANES), 16)
    last_fill = width - (slots - 1) * LANES
    slack = LANES - last_fill
    tail = pl.multiple_of(jnp.maximum(off - slack, 0), 16)
    positions = draft + 1
    halves = batch // SUB
    main = slots - 2
    others = n - 1
    groups = len(plan)

    hcopy = pltpu.make_async_copy(h_ref, hbuf, hsem)
    hcopy.start()
    fcopy = pltpu.make_async_copy(w_ref.at[pl.ds(pl.multiple_of(LANES - off, 16), LANES)], fbuf, hsem)
    fcopy.start()

    barrier = pltpu.get_barrier_semaphore()
    for k in range(1, n):
        pl.semaphore_signal(barrier, inc=1, device_id={AXIS: lax.rem(me + k, n)}, device_id_type=MESH)

    tile_cols = TILE_ROWS * LANES
    tiles = (main - 1) // TILE_ROWS

    def w_copy(t):
        start = pl.multiple_of(2 * LANES - off + t * tile_cols, 16)
        slot = lax.rem(t, NBUF)
        return pltpu.make_async_copy(w_ref.at[pl.ds(start, tile_cols)], wbuf.at[slot], wsem.at[slot])

    w_copy(0).start()
    e1 = pltpu.make_async_copy(w_ref.at[pl.ds(0, LANES)], ebuf.at[pl.ds(pl.multiple_of(LANES + off, 16), LANES)], esem)
    e2 = pltpu.make_async_copy(w_ref.at[pl.ds(width - LANES, LANES)], ebuf.at[pl.ds(tail, LANES)], esem)
    want = (slots - 1) * LANES - off
    src3 = pl.multiple_of(jnp.minimum(want, width - LANES), 16)
    dst3 = pl.multiple_of(3 * LANES + slack + (src3 - want), 16)
    e3 = pltpu.make_async_copy(w_ref.at[pl.ds(src3, LANES)], ebuf.at[pl.ds(dst3, LANES)], esem)
    xcopy = pltpu.make_async_copy(x_hbm, x_ref, xsem)

    hops = []
    for d in range(chips // 2, 0, -1):
        hops += [d] if 2 * d == chips else [d, chips - d]
    order = [(d, c) for c in (1, 0) for d in hops] + [(0, 1)]

    def targets():
        for dz, dc in order:
            yield lax.rem(chip + dz, chips) * 2 + lax.rem(core + dc, 2)

    def send_group(g):
        pos, size = plan[g][:2]
        for k, tgt in enumerate(targets()):
            pltpu.make_async_remote_copy(
                src_ref=send.at[tgt, pl.ds(pos, size), pl.ds(0, positions), :],
                dst_ref=recv.at[me, pl.ds(pos, size), pl.ds(0, positions), :],
                send_sem=ssem, recv_sem=lsem.at[k // LAST_SHARE] if g == groups - 1 else rsem, device_id={AXIS: tgt}, device_id_type=MESH).start()

    send_flat = send.reshape(batch * slots * SUB, LANES)

    def logits_of(block):
        z = lax.dot_general(hbuf[...], block, (((1,), (1,)), ((), ())), preferred_element_type=f32)
        return z * INV_TEMP

    def put(z, pos, ok=None):
        for r in range(positions * halves):
            j, half = r // halves, r % halves
            v = z[r * SUB:(r + 1) * SUB, :]
            send_flat[pl.ds((half * SUB * slots + pos) * SUB + j, SUB, stride=slots * SUB), :] = v
            peak[r] = jnp.maximum(peak[r], v if ok is None else jnp.where(ok, v, jnp.finfo(f32).min))
        recv[me, pos] = send[me, pos]

    peak[...] = jnp.full(peak.shape, jnp.finfo(f32).min, f32)
    both = ebuf.at[pl.ds(0, hbuf.shape[0] + LANES)]
    pltpu.make_async_copy(both, both, hsem).wait()
    w_copy(1).start()
    put(logits_of(fbuf[...]), 0)
    w_copy(2).start()
    e1.start()
    e2.start()
    e3.start()
    xcopy.start()

    lane8 = lax.broadcasted_iota(jnp.int32, (SUB, LANES), 1)
    sub8 = lax.broadcasted_iota(jnp.int32, (SUB, LANES), 0)
    ok_first = jnp.logical_or(lane8 >= off, lane8 < tail)
    ok_last = lane8 < jnp.minimum(off + last_fill, LANES)

    def make_group(g):
        start, _, first, count, has_edge = plan[g]
        if has_edge:
            three = ebuf.at[pl.ds(0, 3 * LANES)]
            pltpu.make_async_copy(three, three, esem).wait()
            put(logits_of(ebuf[pl.ds(LANES, LANES), :]), edge, ok_first)
            put(logits_of(ebuf[pl.ds(3 * LANES + slack, LANES), :]), edge + 1, ok_last)
        base = start + (2 if has_edge else 0) + (1 if g == 0 else 0) - first * TILE_ROWS
        if not count:
            return

        @pl.loop(first, first + count)
        def _(t):
            @pl.when(t + NBUF - 1 < tiles)
            def _():
                w_copy(t + NBUF - 1).start()

            w_copy(t).wait()
            z = logits_of(wbuf[lax.rem(t, NBUF)])
            for i in range(TILE_ROWS):
                put(z[:, i * LANES:(i + 1) * LANES], base + t * TILE_ROWS + i)

    for g in range(groups):
        make_group(g)
        if g == 0:
            pl.semaphore_wait(barrier, n - 1)
        if g < groups - HELD:
            send_group(g)

    for j in range(draft):
        pltpu.make_async_copy(q_ref.at[j, :, 0, :], qbuf.at[:, j, :], qsem).start()

    gap_first = jnp.where(off >= slack, off - 2, LANES)
    gap_last = jnp.where(off >= slack, LANES, LANES - 2)
    for r in range(positions * halves):
        peak_t[pl.ds((r % halves) * SUB * SUB + r // halves, SUB, stride=SUB), :] = peak[r]

    @pl.loop(0, batch)
    def _(b):
        m = jnp.max(peak_t[pl.ds(pl.multiple_of(b * SUB, SUB), SUB), :], axis=1, keepdims=True)
        accs = [jnp.where(ok_first, jnp.exp(send[b, edge] - m), 0.0), jnp.where(ok_last, jnp.exp(send[b, edge + 1] - m), 0.0)] + [0.0] * 2
        for r in [r for r in range(slots) if not edge <= r < edge + 2]:
            accs[r % 4] = accs[r % 4] + jnp.exp(send[b, r] - m)
        l = jnp.sum((accs[0] + accs[1]) + (accs[2] + accs[3]), axis=1, keepdims=True)
        for at, gap in ((edge, gap_first), (edge + 1, gap_last)):
            send[b, at] = jnp.where(lane8 == gap, m, jnp.where(lane8 == gap + 1, l, send[b, at]))

    for at in (edge, edge + 1):
        recv[me, at] = send[me, at]
    for g in range(groups - HELD, groups):
        send_group(g)

    edge_group = next(g for g in range(groups) if plan[g][4])
    assert groups - HELD <= edge_group == groups - 2
    pos, size = plan[groups - 1][:2]
    assert pos + size == slots
    early = recv.at[pl.ds(0, others), pl.ds(0, pos), pl.ds(0, positions), :]
    pltpu.make_async_copy(early, early, rsem).wait()
    stats = []
    for s in range(n):
        o = (s * width) % LANES
        at, gap = (edge, o - 2) if o >= slack else (edge + 1, LANES - 2)
        v = recv[s, at]
        stats.append((v[:, gap:gap + 1], v[:, gap + 1:gap + 2]))
    top = functools.reduce(jnp.maximum, [m for m, _ in stats])
    tot = functools.reduce(jnp.add, [l * jnp.exp(m - top) for m, l in stats])
    peak_g = jnp.broadcast_to(top, (SUB, LANES))
    inv_sum = jnp.broadcast_to(1.0 / tot, (SUB, LANES))

    every = qbuf.at[:, pl.ds(0, draft), :]
    pltpu.make_async_copy(every, every, qsem).wait()
    xcopy.wait()

    is_draft = sub8 < draft

    def excess_of(z, row):
        p = jnp.exp(z - peak_g) * inv_sum
        e = jnp.maximum(p - jnp.where(is_draft, qbuf[row], 0.0), 0.0)
        pe_ref[pl.ds(row, SUB, stride=pitch), :] = e
        return e

    parts = {}
    for s in range(n):
        first, o = (s * width) // LANES, (s * width) % LANES
        t_s = max(o - slack, 0)
        parts.setdefault(first, []).append((s, edge, o, LANES))
        if t_s:
            parts.setdefault(first + slots, []).append((s, edge, 0, t_s))
        parts.setdefault(first + slots - 1, []).append((s, edge + 1, 0, min(LANES, o + last_fill)))

    here, where, q_at = [], [], jnp.ones((SUB, LANES), f32)
    for j in range(draft):
        x = x_ref[j, me]
        s = x // width
        row = x // LANES
        slot = row - (s * width) // LANES
        at = jnp.where(slot <= edge, slot - 1, slot + 1)
        at = jnp.where(jnp.logical_or(slot == 0, slot == slots), edge, jnp.where(slot == slots - 1, edge + 1, at))
        where.append((s, at))
        here.append(jnp.logical_and(sub8 == j, lane8 == lax.rem(x, LANES)))
        q_at = jnp.where(here[j], qbuf[row], q_at)
    spare = pitch - SUB
    chosen = functools.reduce(jnp.logical_or, here)
    for i, v in enumerate((q_at, jnp.where(chosen, 1.0, 0.0), peak_g, inv_sum)):
        pe_ref[pl.ds((2 + i) * pitch + spare, SUB), :] = v

    def rows_of(s, pos, size, acc):
        base = (s * width) // LANES + pos + (1 if pos < edge else -1)
        es = [excess_of(recv[s, pos + i], base + i) for i in range(size)]
        while len(es) > 1:
            es = [es[i] + es[i + 1] for i in range(0, len(es) - 1, 2)] + ([es[-1]] if len(es) % 2 else [])
        return acc + es[0]

    acc = jnp.zeros((SUB, LANES), f32)
    for g in range(groups - 1):
        pos, size, _, _, has_edge = plan[g]
        if has_edge:
            for row, pieces in sorted(parts.items()):
                z = recv[pieces[0][0], pieces[0][1]]
                for s, at, lo, hi in pieces[1:]:
                    z = jnp.where(jnp.logical_and(lane8 >= lo, lane8 < hi), recv[s, at], z)
                acc = acc + excess_of(z, row)
            pos, size = pos + 2, size - 2
        if size:
            acc = lax.fori_loop(0, n, functools.partial(lambda s, acc, pos, size: rows_of(s, pos, size, acc), pos=pos, size=size), acc)

    pos, size = plan[groups - 1][:2]
    acc = rows_of(me, pos, size, acc)
    for k, (dz, dc) in enumerate(order):
        if k % LAST_SHARE == 0:
            view = recv.at[pl.ds(0, min(LAST_SHARE, others - k)), pl.ds(pos, size), pl.ds(0, positions), :]
            pltpu.make_async_copy(view, view, lsem.at[k // LAST_SHARE]).wait()
        acc = rows_of(lax.rem(chip - dz + chips, chips) * 2 + lax.rem(core + dc, 2), pos, size, acc)
    pe_ref[pl.ds(spare, SUB), :] = jnp.broadcast_to(1.0 / jnp.sum(acc, axis=1, keepdims=True), (SUB, LANES))
    z_at = jnp.zeros((SUB, LANES), f32)
    for j in range(draft):
        z_at = jnp.where(here[j], recv[where[j][0], where[j][1]], z_at)
    pe_ref[pl.ds(pitch + spare, SUB), :] = z_at

    sent = send.at[pl.ds(0, others), :, pl.ds(0, positions), :]
    pltpu.make_async_copy(sent, sent, ssem).wait()


def finish_kernel(geo, pe_ref, res_ref, bonus_ref, acc_hbm, exp_hbm, stage, acc_ref, exp_ref, sem, small):
    total_rows, pitch, draft, cuts = geo
    copies = [pltpu.make_async_copy(pe_ref.at[pl.ds(draft * pitch, total_rows), :], bonus_ref.at[:, 0, :], sem)]
    copies[0].start()
    spare = pitch - SUB
    for j in range(draft):
        scale = jnp.broadcast_to(pe_ref[spare + j:spare + j + 1, :], (SUB, LANES))
        for lo, hi in cuts:
            up = -(-hi // SUB) * SUB
            block = pe_ref[j * pitch + lo:j * pitch + up, :].reshape((up - lo) // SUB, SUB, LANES)
            stage[j, lo:up, :] = (block * scale[None]).reshape(up - lo, LANES)
            copies.append(pltpu.make_async_copy(stage.at[j, pl.ds(lo, hi - lo), :], res_ref.at[j, pl.ds(lo, hi - lo), 0, :], sem))
            copies[-1].start()
    z_at, q_at, chosen, peak_g, inv_sum = (pe_ref[(1 + i) * pitch + spare:(2 + i) * pitch, :] for i in range(5))
    ratio = jnp.minimum(1.0, jnp.exp(z_at - peak_g) * inv_sum / q_at)
    accept = jnp.sum(jnp.where(chosen > 0.5, ratio, 0.0), axis=1, keepdims=True)
    lane8 = lax.broadcasted_iota(jnp.int32, (SUB, LANES), 1)
    sub8 = lax.broadcasted_iota(jnp.int32, (SUB, LANES), 0)
    acc_ref[...] = jnp.sum(jnp.where(lane8 == sub8, accept, 0.0), axis=0, keepdims=True)[:, :draft]
    prod = accept[0:1, :]
    expect = prod
    for j in range(1, draft):
        prod = prod * accept[j:j + 1, :]
        expect = expect + prod
    exp_ref[...] = expect
    acc_copy = pltpu.make_async_copy(acc_ref, acc_hbm, small.at[0])
    exp_copy = pltpu.make_async_copy(exp_ref, exp_hbm, small.at[1])
    acc_copy.start()
    exp_copy.start()
    whole = pe_ref.at[pl.ds(0, (draft + 1) * total_rows), :]
    pltpu.make_async_copy(whole, whole, sem).wait()
    acc_copy.wait()
    exp_copy.wait()


def solution(mesh):
    n = mesh.shape[AXIS]

    def local_step(hidden, w_shard, q_rows, x_group):
        f32 = jnp.float32
        batch, positions, depth = hidden.shape
        draft = positions - 1
        width = w_shard.shape[1]
        vocab = q_rows.shape[2]
        slots = -(-width // LANES)
        total_rows = vocab // LANES
        padded = -(-total_rows // SUB) * SUB
        pitch = padded + SUB
        slack = slots * LANES - width
        plan, edge = group_plan(slots)
        h = jnp.transpose(hidden, (1, 0, 2)).reshape(positions * batch, depth)
        w = jnp.transpose(w_shard)
        q = jnp.transpose(q_rows, (1, 0, 2)).reshape(draft, total_rows, 1, LANES)
        x = jnp.transpose(x_group)
        hbm = pl.BlockSpec(memory_space=pltpu.HBM)
        vmem = pl.BlockSpec(memory_space=pltpu.VMEM)
        w, h, q, x = (pltpu.with_memory_space_constraint(a, pltpu.HBM) for a in (w, h, q, x))
        geo = (n, width, slots, draft, batch, total_rows, pitch, plan, edge)
        pe = pl.pallas_call(
            functools.partial(exchange_kernel, geo),
            name="verify_exchange",
            out_shape=jax.ShapeDtypeStruct((SUB * pitch, LANES), f32),
            in_specs=[hbm, hbm, hbm, hbm],
            out_specs=vmem,
            scratch_shapes=[
                pltpu.SMEM((draft, batch), jnp.int32),
                pltpu.VMEM((positions * batch, depth), jnp.bfloat16),
                pltpu.VMEM((LANES, depth), jnp.bfloat16),
                pltpu.VMEM((4 * LANES + slack, depth), jnp.bfloat16),
                pltpu.VMEM((NBUF, TILE_ROWS * LANES, depth), jnp.bfloat16),
                pltpu.VMEM((batch, slots, SUB, LANES), f32),
                pltpu.VMEM((n, slots, SUB, LANES), f32),
                pltpu.VMEM((total_rows, SUB, LANES), f32),
                pltpu.VMEM((positions * batch // SUB, SUB, LANES), f32),
                pltpu.VMEM((batch * SUB, LANES), f32),
                pltpu.SemaphoreType.DMA,
                pltpu.SemaphoreType.DMA,
                pltpu.SemaphoreType.DMA,
                pltpu.SemaphoreType.DMA((NBUF,)),
                pltpu.SemaphoreType.DMA,
                pltpu.SemaphoreType.DMA,
                pltpu.SemaphoreType.DMA,
                pltpu.SemaphoreType.DMA((-(-(n - 1) // LAST_SHARE),)),
            ],
            compiler_params=pltpu.CompilerParams(collective_id=0, has_side_effects=True, vmem_limit_bytes=40 * 2**20),
        )(w, h, q, x)
        cuts = ((0, total_rows),)
        res, bonus, accept, expected = pl.pallas_call(
            functools.partial(finish_kernel, (total_rows, pitch, draft, cuts)),
            name="verify_finish",
            out_shape=(jax.ShapeDtypeStruct((draft, total_rows, 1, LANES), f32),
                       jax.ShapeDtypeStruct((total_rows, 1, LANES), f32),
                       jax.ShapeDtypeStruct((1, draft), f32),
                       jax.ShapeDtypeStruct((1, 1), f32)),
            in_specs=[vmem],
            out_specs=(hbm, hbm, hbm, hbm),
            scratch_shapes=[pltpu.VMEM((draft, padded, LANES), f32), pltpu.VMEM((1, draft), f32), pltpu.VMEM((1, 1), f32),
                            pltpu.SemaphoreType.DMA, pltpu.SemaphoreType.DMA((2,))],
            compiler_params=pltpu.CompilerParams(vmem_limit_bytes=16 * 2**20),
        )(pe)
        residual = jnp.transpose(res.reshape(draft, 1, vocab), (1, 0, 2))
        return accept, expected.reshape(1), residual, bonus.reshape(1, vocab)

    return jax.shard_map(local_step, mesh=mesh,
                         in_specs=(P("dp", None, None), P(None, AXIS), P(("dp", AXIS), None, None), P("dp", None)),
                         out_specs=(P(("dp", AXIS), None), P(("dp", AXIS)), P(("dp", AXIS), None, None), P(("dp", AXIS), None)),
                         check_vma=False)
```

```python
import functools

import jax
import jax.numpy as jnp
from jax import lax
from jax.experimental import pallas as pl
from jax.experimental.pallas import tpu as pltpu
from jax.sharding import PartitionSpec as P

INV_TEMP = 1.25
LANES = 128
SUB = 8
TILE_ROWS = 2
NBUF = 4
AXIS = "tp"
MESH = pl.DeviceIdType.MESH


GROUPS = (("F",), (1,), (1,), (2,), (4,), (8,), ("E", 9), (5,))
HELD = 2
LAST_SHARE = 4


def group_plan(slots):
    pos = tile = 0
    edge = None
    plan = []
    for group in GROUPS:
        start, first, has_edge = pos, tile, False
        for item in group:
            if item == "F":
                assert pos == 0
                pos += 1
            elif item == "E":
                assert pos == start
                edge, has_edge = pos, True
                pos += 2
            else:
                tile += item
                pos += item * TILE_ROWS
        plan.append((start, pos - start, first, tile - first, has_edge))
    assert pos == slots and edge is not None
    return tuple(plan), edge


def exchange_kernel(geo, w_ref, h_ref, q_ref, x_hbm, pe_ref,
                    x_ref, hbuf, fbuf, ebuf, wbuf, send, recv, qbuf, peak, peak_t,
                    xsem, hsem, esem, wsem, qsem, ssem, rsem, lsem):
    n, width, slots, draft, batch, total_rows, pitch, plan, edge = geo
    f32 = jnp.float32
    me = lax.axis_index(AXIS)
    chip, core = me // 2, lax.rem(me, 2)
    chips = n // 2
    off = pl.multiple_of(lax.rem(me * width, LANES), 16)
    last_fill = width - (slots - 1) * LANES
    slack = LANES - last_fill
    tail = pl.multiple_of(jnp.maximum(off - slack, 0), 16)
    positions = draft + 1
    halves = batch // SUB
    main = slots - 2
    others = n - 1
    groups = len(plan)

    hcopy = pltpu.make_async_copy(h_ref, hbuf, hsem)
    hcopy.start()
    fcopy = pltpu.make_async_copy(w_ref.at[pl.ds(pl.multiple_of(LANES - off, 16), LANES)], fbuf, hsem)
    fcopy.start()

    barrier = pltpu.get_barrier_semaphore()
    for k in range(1, n):
        pl.semaphore_signal(barrier, inc=1, device_id={AXIS: lax.rem(me + k, n)}, device_id_type=MESH)

    tile_cols = TILE_ROWS * LANES
    tiles = (main - 1) // TILE_ROWS

    def w_copy(t):
        start = pl.multiple_of(2 * LANES - off + t * tile_cols, 16)
        slot = lax.rem(t, NBUF)
        return pltpu.make_async_copy(w_ref.at[pl.ds(start, tile_cols)], wbuf.at[slot], wsem.at[slot])

    w_copy(0).start()
    e1 = pltpu.make_async_copy(w_ref.at[pl.ds(0, LANES)], ebuf.at[pl.ds(pl.multiple_of(LANES + off, 16), LANES)], esem)
    e2 = pltpu.make_async_copy(w_ref.at[pl.ds(width - LANES, LANES)], ebuf.at[pl.ds(tail, LANES)], esem)
    want = (slots - 1) * LANES - off
    src3 = pl.multiple_of(jnp.minimum(want, width - LANES), 16)
    dst3 = pl.multiple_of(3 * LANES + slack + (src3 - want), 16)
    e3 = pltpu.make_async_copy(w_ref.at[pl.ds(src3, LANES)], ebuf.at[pl.ds(dst3, LANES)], esem)
    xcopy = pltpu.make_async_copy(x_hbm, x_ref, xsem)

    hops = []
    for d in range(chips // 2, 0, -1):
        hops += [d] if 2 * d == chips else [d, chips - d]
    order = [(d, c) for c in (1, 0) for d in hops] + [(0, 1)]

    def targets():
        for dz, dc in order:
            yield lax.rem(chip + dz, chips) * 2 + lax.rem(core + dc, 2)

    def send_group(g):
        pos, size = plan[g][:2]
        for k, tgt in enumerate(targets()):
            pltpu.make_async_remote_copy(
                src_ref=send.at[tgt, pl.ds(pos, size), pl.ds(0, positions), :],
                dst_ref=recv.at[me, pl.ds(pos, size), pl.ds(0, positions), :],
                send_sem=ssem, recv_sem=lsem.at[k // LAST_SHARE] if g == groups - 1 else rsem, device_id={AXIS: tgt}, device_id_type=MESH).start()

    send_flat = send.reshape(batch * slots * SUB, LANES)

    def logits_of(block):
        z = lax.dot_general(hbuf[...], block, (((1,), (1,)), ((), ())), preferred_element_type=f32)
        return z * INV_TEMP

    def put(z, pos, ok=None):
        for r in range(positions * halves):
            j, half = r // halves, r % halves
            v = z[r * SUB:(r + 1) * SUB, :]
            send_flat[pl.ds((half * SUB * slots + pos) * SUB + j, SUB, stride=slots * SUB), :] = v
            peak[r] = jnp.maximum(peak[r], v if ok is None else jnp.where(ok, v, jnp.finfo(f32).min))
        recv[me, pos] = send[me, pos]

    peak[...] = jnp.full(peak.shape, jnp.finfo(f32).min, f32)
    both = ebuf.at[pl.ds(0, hbuf.shape[0] + LANES)]
    pltpu.make_async_copy(both, both, hsem).wait()
    w_copy(1).start()
    put(logits_of(fbuf[...]), 0)
    w_copy(2).start()
    e1.start()
    e2.start()
    e3.start()
    xcopy.start()

    lane8 = lax.broadcasted_iota(jnp.int32, (SUB, LANES), 1)
    sub8 = lax.broadcasted_iota(jnp.int32, (SUB, LANES), 0)
    ok_first = jnp.logical_or(lane8 >= off, lane8 < tail)
    ok_last = lane8 < jnp.minimum(off + last_fill, LANES)

    def make_group(g):
        start, _, first, count, has_edge = plan[g]
        if has_edge:
            three = ebuf.at[pl.ds(0, 3 * LANES)]
            pltpu.make_async_copy(three, three, esem).wait()
            put(logits_of(ebuf[pl.ds(LANES, LANES), :]), edge, ok_first)
            put(logits_of(ebuf[pl.ds(3 * LANES + slack, LANES), :]), edge + 1, ok_last)
        base = start + (2 if has_edge else 0) + (1 if g == 0 else 0) - first * TILE_ROWS
        if not count:
            return

        @pl.loop(first, first + count)
        def _(t):
            @pl.when(t + NBUF - 1 < tiles)
            def _():
                w_copy(t + NBUF - 1).start()

            w_copy(t).wait()
            z = logits_of(wbuf[lax.rem(t, NBUF)])
            for i in range(TILE_ROWS):
                put(z[:, i * LANES:(i + 1) * LANES], base + t * TILE_ROWS + i)

    for g in range(groups):
        make_group(g)
        if g == 0:
            pl.semaphore_wait(barrier, n - 1)
        if g < groups - HELD:
            send_group(g)

    for j in range(draft):
        pltpu.make_async_copy(q_ref.at[j, :, 0, :], qbuf.at[:, j, :], qsem).start()

    gap_first = jnp.where(off >= slack, off - 2, LANES)
    gap_last = jnp.where(off >= slack, LANES, LANES - 2)
    for r in range(positions * halves):
        peak_t[pl.ds((r % halves) * SUB * SUB + r // halves, SUB, stride=SUB), :] = peak[r]

    @pl.loop(0, batch)
    def _(b):
        m = jnp.max(peak_t[pl.ds(pl.multiple_of(b * SUB, SUB), SUB), :], axis=1, keepdims=True)
        accs = [jnp.where(ok_first, jnp.exp(send[b, edge] - m), 0.0), jnp.where(ok_last, jnp.exp(send[b, edge + 1] - m), 0.0)] + [0.0] * 2
        for r in [r for r in range(slots) if not edge <= r < edge + 2]:
            accs[r % 4] = accs[r % 4] + jnp.exp(send[b, r] - m)
        l = jnp.sum((accs[0] + accs[1]) + (accs[2] + accs[3]), axis=1, keepdims=True)
        for at, gap in ((edge, gap_first), (edge + 1, gap_last)):
            send[b, at] = jnp.where(lane8 == gap, m, jnp.where(lane8 == gap + 1, l, send[b, at]))

    for at in (edge, edge + 1):
        recv[me, at] = send[me, at]
    for g in range(groups - HELD, groups):
        send_group(g)

    edge_group = next(g for g in range(groups) if plan[g][4])
    assert groups - HELD <= edge_group == groups - 2
    pos, size = plan[groups - 1][:2]
    assert pos + size == slots
    early = recv.at[pl.ds(0, others), pl.ds(0, pos), pl.ds(0, positions), :]
    pltpu.make_async_copy(early, early, rsem).wait()
    stats = []
    for s in range(n):
        o = (s * width) % LANES
        at, gap = (edge, o - 2) if o >= slack else (edge + 1, LANES - 2)
        v = recv[s, at]
        stats.append((v[:, gap:gap + 1], v[:, gap + 1:gap + 2]))
    top = functools.reduce(jnp.maximum, [m for m, _ in stats])
    tot = functools.reduce(jnp.add, [l * jnp.exp(m - top) for m, l in stats])
    peak_g = jnp.broadcast_to(top, (SUB, LANES))
    inv_sum = jnp.broadcast_to(1.0 / tot, (SUB, LANES))

    every = qbuf.at[:, pl.ds(0, draft), :]
    pltpu.make_async_copy(every, every, qsem).wait()
    xcopy.wait()

    is_draft = sub8 < draft

    def excess_of(z, row):
        p = jnp.exp(z - peak_g) * inv_sum
        e = jnp.maximum(p - jnp.where(is_draft, qbuf[row], 0.0), 0.0)
        pe_ref[pl.ds(row, SUB, stride=pitch), :] = e
        return e

    parts = {}
    for s in range(n):
        first, o = (s * width) // LANES, (s * width) % LANES
        t_s = max(o - slack, 0)
        parts.setdefault(first, []).append((s, edge, o, LANES))
        if t_s:
            parts.setdefault(first + slots, []).append((s, edge, 0, t_s))
        parts.setdefault(first + slots - 1, []).append((s, edge + 1, 0, min(LANES, o + last_fill)))

    here, where, q_at = [], [], jnp.ones((SUB, LANES), f32)
    for j in range(draft):
        x = x_ref[j, me]
        s = x // width
        row = x // LANES
        slot = row - (s * width) // LANES
        at = jnp.where(slot <= edge, slot - 1, slot + 1)
        at = jnp.where(jnp.logical_or(slot == 0, slot == slots), edge, jnp.where(slot == slots - 1, edge + 1, at))
        where.append((s, at))
        here.append(jnp.logical_and(sub8 == j, lane8 == lax.rem(x, LANES)))
        q_at = jnp.where(here[j], qbuf[row], q_at)
    spare = pitch - SUB
    chosen = functools.reduce(jnp.logical_or, here)
    for i, v in enumerate((q_at, jnp.where(chosen, 1.0, 0.0), peak_g, inv_sum)):
        pe_ref[pl.ds((2 + i) * pitch + spare, SUB), :] = v

    def rows_of(s, pos, size, acc):
        base = (s * width) // LANES + pos + (1 if pos < edge else -1)
        es = [excess_of(recv[s, pos + i], base + i) for i in range(size)]
        while len(es) > 1:
            es = [es[i] + es[i + 1] for i in range(0, len(es) - 1, 2)] + ([es[-1]] if len(es) % 2 else [])
        return acc + es[0]

    acc = jnp.zeros((SUB, LANES), f32)
    for g in range(groups - 1):
        pos, size, _, _, has_edge = plan[g]
        if has_edge:
            for row, pieces in sorted(parts.items()):
                z = recv[pieces[0][0], pieces[0][1]]
                for s, at, lo, hi in pieces[1:]:
                    z = jnp.where(jnp.logical_and(lane8 >= lo, lane8 < hi), recv[s, at], z)
                acc = acc + excess_of(z, row)
            pos, size = pos + 2, size - 2
        if size:
            acc = lax.fori_loop(0, n, functools.partial(lambda s, acc, pos, size: rows_of(s, pos, size, acc), pos=pos, size=size), acc)

    pos, size = plan[groups - 1][:2]
    acc = rows_of(me, pos, size, acc)
    for k, (dz, dc) in enumerate(order):
        if k % LAST_SHARE == 0:
            view = recv.at[pl.ds(0, min(LAST_SHARE, others - k)), pl.ds(pos, size), pl.ds(0, positions), :]
            pltpu.make_async_copy(view, view, lsem.at[k // LAST_SHARE]).wait()
        acc = rows_of(lax.rem(chip - dz + chips, chips) * 2 + lax.rem(core + dc, 2), pos, size, acc)
    pe_ref[pl.ds(spare, SUB), :] = jnp.broadcast_to(1.0 / jnp.sum(acc, axis=1, keepdims=True), (SUB, LANES))
    z_at = jnp.zeros((SUB, LANES), f32)
    for j in range(draft):
        z_at = jnp.where(here[j], recv[where[j][0], where[j][1]], z_at)
    pe_ref[pl.ds(pitch + spare, SUB), :] = z_at

    sent = send.at[pl.ds(0, others), :, pl.ds(0, positions), :]
    pltpu.make_async_copy(sent, sent, ssem).wait()


def finish_kernel(geo, pe_ref, res_ref, bonus_ref, acc_hbm, exp_hbm, stage, acc_ref, exp_ref, sem, small):
    total_rows, pitch, draft, cuts = geo
    copies = [pltpu.make_async_copy(pe_ref.at[pl.ds(draft * pitch, total_rows), :], bonus_ref.at[:, 0, :], sem)]
    copies[0].start()
    spare = pitch - SUB
    for j in range(draft):
        scale = jnp.broadcast_to(pe_ref[spare + j:spare + j + 1, :], (SUB, LANES))
        for lo, hi in cuts:
            up = -(-hi // SUB) * SUB
            block = pe_ref[j * pitch + lo:j * pitch + up, :].reshape((up - lo) // SUB, SUB, LANES)
            stage[j, lo:up, :] = (block * scale[None]).reshape(up - lo, LANES)
            copies.append(pltpu.make_async_copy(stage.at[j, pl.ds(lo, hi - lo), :], res_ref.at[j, pl.ds(lo, hi - lo), 0, :], sem))
            copies[-1].start()
    z_at, q_at, chosen, peak_g, inv_sum = (pe_ref[(1 + i) * pitch + spare:(2 + i) * pitch, :] for i in range(5))
    ratio = jnp.minimum(1.0, jnp.exp(z_at - peak_g) * inv_sum / q_at)
    accept = jnp.sum(jnp.where(chosen > 0.5, ratio, 0.0), axis=1, keepdims=True)
    lane8 = lax.broadcasted_iota(jnp.int32, (SUB, LANES), 1)
    sub8 = lax.broadcasted_iota(jnp.int32, (SUB, LANES), 0)
    acc_ref[...] = jnp.sum(jnp.where(lane8 == sub8, accept, 0.0), axis=0, keepdims=True)[:, :draft]
    prod = accept[0:1, :]
    expect = prod
    for j in range(1, draft):
        prod = prod * accept[j:j + 1, :]
        expect = expect + prod
    exp_ref[...] = expect
    acc_copy = pltpu.make_async_copy(acc_ref, acc_hbm, small.at[0])
    exp_copy = pltpu.make_async_copy(exp_ref, exp_hbm, small.at[1])
    acc_copy.start()
    exp_copy.start()
    whole = pe_ref.at[pl.ds(0, (draft + 1) * total_rows), :]
    pltpu.make_async_copy(whole, whole, sem).wait()
    acc_copy.wait()
    exp_copy.wait()


def solution(mesh):
    n = mesh.shape[AXIS]

    def local_step(hidden, w_shard, q_rows, x_group):
        f32 = jnp.float32
        batch, positions, depth = hidden.shape
        draft = positions - 1
        width = w_shard.shape[1]
        vocab = q_rows.shape[2]
        slots = -(-width // LANES)
        total_rows = vocab // LANES
        padded = -(-total_rows // SUB) * SUB
        pitch = padded + SUB
        slack = slots * LANES - width
        plan, edge = group_plan(slots)
        h = jnp.transpose(hidden, (1, 0, 2)).reshape(positions * batch, depth)
        w = jnp.transpose(w_shard)
        q = jnp.transpose(q_rows, (1, 0, 2)).reshape(draft, total_rows, 1, LANES)
        x = jnp.transpose(x_group)
        hbm = pl.BlockSpec(memory_space=pltpu.HBM)
        vmem = pl.BlockSpec(memory_space=pltpu.VMEM)
        w, h, q, x = (pltpu.with_memory_space_constraint(a, pltpu.HBM) for a in (w, h, q, x))
        geo = (n, width, slots, draft, batch, total_rows, pitch, plan, edge)
        pe = pl.pallas_call(
            functools.partial(exchange_kernel, geo),
            name="verify_exchange",
            out_shape=jax.ShapeDtypeStruct((SUB * pitch, LANES), f32),
            in_specs=[hbm, hbm, hbm, hbm],
            out_specs=vmem,
            scratch_shapes=[
                pltpu.SMEM((draft, batch), jnp.int32),
                pltpu.VMEM((positions * batch, depth), jnp.bfloat16),
                pltpu.VMEM((LANES, depth), jnp.bfloat16),
                pltpu.VMEM((4 * LANES + slack, depth), jnp.bfloat16),
                pltpu.VMEM((NBUF, TILE_ROWS * LANES, depth), jnp.bfloat16),
                pltpu.VMEM((batch, slots, SUB, LANES), f32),
                pltpu.VMEM((n, slots, SUB, LANES), f32),
                pltpu.VMEM((total_rows, SUB, LANES), f32),
                pltpu.VMEM((positions * batch // SUB, SUB, LANES), f32),
                pltpu.VMEM((batch * SUB, LANES), f32),
                pltpu.SemaphoreType.DMA,
                pltpu.SemaphoreType.DMA,
                pltpu.SemaphoreType.DMA,
                pltpu.SemaphoreType.DMA((NBUF,)),
                pltpu.SemaphoreType.DMA,
                pltpu.SemaphoreType.DMA,
                pltpu.SemaphoreType.DMA,
                pltpu.SemaphoreType.DMA((-(-(n - 1) // LAST_SHARE),)),
            ],
            compiler_params=pltpu.CompilerParams(collective_id=0, has_side_effects=True, vmem_limit_bytes=40 * 2**20),
        )(w, h, q, x)
        cuts = ((0, total_rows),)
        res, bonus, accept, expected = pl.pallas_call(
            functools.partial(finish_kernel, (total_rows, pitch, draft, cuts)),
            name="verify_finish",
            out_shape=(jax.ShapeDtypeStruct((draft, total_rows, 1, LANES), f32),
                       jax.ShapeDtypeStruct((total_rows, 1, LANES), f32),
                       jax.ShapeDtypeStruct((1, draft), f32),
                       jax.ShapeDtypeStruct((1, 1), f32)),
            in_specs=[vmem],
            out_specs=(hbm, hbm, hbm, hbm),
            scratch_shapes=[pltpu.VMEM((draft, padded, LANES), f32), pltpu.VMEM((1, draft), f32), pltpu.VMEM((1, 1), f32),
                            pltpu.SemaphoreType.DMA, pltpu.SemaphoreType.DMA((2,))],
            compiler_params=pltpu.CompilerParams(vmem_limit_bytes=16 * 2**20),
        )(pe)
        residual = jnp.transpose(res.reshape(draft, 1, vocab), (1, 0, 2))
        return accept, expected.reshape(1), residual, bonus.reshape(1, vocab)

    return jax.shard_map(local_step, mesh=mesh,
                         in_specs=(P("dp", None, None), P(None, AXIS), P(("dp", AXIS), None, None), P("dp", None)),
                         out_specs=(P(("dp", AXIS), None), P(("dp", AXIS)), P(("dp", AXIS), None, None), P(("dp", AXIS), None)),
                         check_vma=False)
```
